32 devices in a mesh: leaf: 8 (over z, y), rhs: 4 (over x, core).
Axes of the slice: x: 2, y: 2, z: 4, core: 2. Of those that a mesh axis runs over, the one named last changes fastest.
Arguments:
- right_sides: float32 [64, 8192], P('rhs', 'leaf'), may hold values from -8 to 8
- leaf_inverse: float32 [8192, 1024], P('leaf', 'rhs'), may hold values from -1 to 5, as said below
- bases: bfloat16 [3, 128, 8192], P(None, None, 'leaf'), may hold values from -1 to 1
- ordering: int32 [8, 1024], P('leaf'), may hold values from 0 to 1023, as said below
Outputs:
- solution: float32 [64, 8192], P('rhs', 'leaf')
The draws below stay inside these ranges and needn't reach their ends.
Inputs may be any that keep to these rules, and one draw needn't show every extreme that they name: `leaf_inverse`: each leaf's block of 1024 rows is symmetric positive definite. `ordering`: each row is a permutation of 0 to 1023.
All inputs are finite; a program needn't handle non-finite values.
Results may differ from the reference program's by a relative error of at most 0.0003.
Values sent between devices are 32-bit elements; how exact they have to be, the bound alone decides.
A program may use at most 64 MiB of HBM per device.

```python
import math
import jax
import jax.numpy as jnp
from jax import lax

LEAF = 1024
R = 128
RHS = 64
LEVELS = 3
NPTS = 8192
N_LEAF = 8


def basis_and_order(key):
    order_key = jax.random.fold_in(key, 7)
    leaf_keys = jax.random.split(order_key, N_LEAF)
    ordering = jax.vmap(lambda single: jax.random.permutation(single, LEAF))(leaf_keys).astype(jnp.int32)
    noise_key = jax.random.fold_in(key, 11)
    heights = jnp.arange(1, LEVELS + 1, dtype=jnp.float32)
    scales = 2.0 / jnp.sqrt(LEAF * 2.0 ** heights)
    noise = jax.random.normal(noise_key, (LEVELS, R, NPTS))
    basis_rows = jnp.clip(noise * scales[:, None, None], -1.0, 1.0)
    return (basis_rows, ordering)


def draw_bases(key, part):
    return basis_and_order(key)[0].astype(jnp.bfloat16)


def draw_ordering(key, part):
    return basis_and_order(key)[1]


def draw_right_sides(key, part):
    basis_rows, ordering = basis_and_order(key)
    tree_order = jnp.zeros((RHS, NPTS), jnp.float32)
    for height in range(LEVELS):
        node_span = LEAF * 2 ** (height + 1)
        groups = NPTS // node_span
        spread = (node_span / (4.0 * R)) ** 0.5
        mixing = jax.random.normal(jax.random.fold_in(key, 40 + height), (groups, R, RHS)) * spread
        level_term = jnp.einsum('rns,nrk->kns', basis_rows[height].reshape(R, groups, node_span), mixing)
        tree_order = tree_order + level_term.reshape(RHS, NPTS)
    tree_order = 0.5 * tree_order + 0.5 * jax.random.normal(jax.random.fold_in(key, 50), (RHS, NPTS))
    tree_order = jnp.clip(tree_order, -8.0, 8.0)
    by_leaf = tree_order.reshape(RHS, N_LEAF, LEAF)
    leaf_ids = jnp.arange(N_LEAF, dtype=jnp.int32)[:, None]
    data_order = jnp.zeros_like(by_leaf).at[:, leaf_ids, ordering].set(by_leaf)
    return data_order.reshape(RHS, NPTS)


def draw_leaf_inverse(key, part):
    diag_key = jax.random.fold_in(key, 21)
    off_key = jax.random.fold_in(key, 22)
    diagonal = jnp.exp(jax.random.uniform(diag_key, (N_LEAF, LEAF), minval=math.log(0.5), maxval=math.log(2.0)))
    raw_values = jnp.clip(jax.random.normal(off_key, (N_LEAF, LEAF, LEAF)), -3.0, 3.0)
    off_part = (raw_values + jnp.transpose(raw_values, (0, 2, 1))) * (0.2 / math.sqrt(2.0 * LEAF))
    matrix = off_part + diagonal[:, :, None] * jnp.eye(LEAF, dtype=jnp.float32)
    return jnp.clip(matrix, -1.0, 5.0).reshape(NPTS, LEAF)


def setup_inputs(seed: int = 0) -> dict:
    splits = jax.random.split(jax.random.key(seed), 5)
    return {
        "right_sides": draw_right_sides(jax.random.fold_in(splits[4], 71), 0),
        "leaf_inverse": draw_leaf_inverse(jax.random.fold_in(splits[4], 71), 0),
        "bases": draw_bases(jax.random.fold_in(splits[4], 71), 0),
        "ordering": draw_ordering(jax.random.fold_in(splits[4], 71), 0),
    }


def solve_factor(factor, values):
    middle = lax.linalg.triangular_solve(factor, values, left_side=True, lower=True)
    return lax.linalg.triangular_solve(factor, middle, left_side=True, lower=True, transpose_a=True)

def reference(right_sides, leaf_inverse, bases, ordering):
    highest = lax.Precision.HIGHEST
    by_leaf = right_sides.reshape(RHS, N_LEAF, LEAF)
    tree_order = jnp.take_along_axis(by_leaf, ordering[None, :, :], axis=2)
    basis_rows = bases.astype(jnp.float32)
    stacked = jnp.concatenate([tree_order, basis_rows.reshape(LEVELS * R, N_LEAF, LEAF)], 0)
    inverses = leaf_inverse.reshape(N_LEAF, LEAF, LEAF)
    applied = jnp.einsum('cip,iqp->ciq', stacked, inverses, precision=highest)
    applied = applied.reshape(RHS + LEVELS * R, NPTS)
    solved = applied[:RHS]
    pending = [applied[RHS + offset * R:RHS + (offset + 1) * R] for offset in range(LEVELS)]
    for height in range(LEVELS):
        node_span = LEAF * 2 ** (height + 1)
        groups = NPTS // node_span
        level_basis = basis_rows[height].reshape(R, groups, node_span)
        level_solved = pending[height].reshape(R, groups, node_span)
        carried = jnp.concatenate([solved] + pending[height + 1:], 0)
        column_count = carried.shape[0]
        grouped = carried.reshape(column_count, groups, node_span)
        capacity = jnp.einsum('rgp,sgp->grs', level_basis, level_solved, precision=highest)
        capacity = capacity + jnp.eye(R, dtype=jnp.float32)
        projected = jnp.einsum('rgp,cgp->grc', level_basis, grouped, precision=highest)
        factor = jnp.linalg.cholesky(capacity)
        weights = solve_factor(factor, projected)
        grouped = grouped - jnp.einsum('grc,rgp->cgp', weights, level_solved, precision=highest)
        carried = grouped.reshape(column_count, NPTS)
        solved = carried[:RHS]
        later = [carried[RHS + offset * R:RHS + (offset + 1) * R] for offset in range(LEVELS - height - 1)]
        pending = pending[:height + 1] + later
    untangled = solved.reshape(RHS, N_LEAF, LEAF)
    leaf_ids = jnp.arange(N_LEAF, dtype=jnp.int32)[:, None]
    result = jnp.zeros_like(untangled).at[:, leaf_ids, ordering].set(untangled)
    return result.reshape(RHS, NPTS)
```

```python
import functools

import jax
import jax.numpy as jnp
from jax import lax
from jax.experimental import pallas as pl
from jax.experimental.pallas import tpu as pltpu
from jax.sharding import PartitionSpec as P

F32 = jnp.float32
BF16 = jnp.bfloat16
NN = (((1,), (0,)), ((), ()))
NT = (((1,), (1,)), ((), ()))
PANEL = 16


def split(value, pieces):
    parts = []
    for _ in range(pieces):
        head = value.astype(BF16)
        parts.append(head)
        value = value - head.astype(F32)
    return parts


def dot(left, right, dims):
    return lax.dot_general(left, right, dims, preferred_element_type=F32)


def fine(left, right, dims):
    return lax.dot_general(
        left, right, dims, precision=lax.Precision.HIGHEST, preferred_element_type=F32
    )


def inverse(matrix):
    size = matrix.shape[0]
    count = size // PANEL
    lane = lax.broadcasted_iota(jnp.int32, (PANEL, size), 1)
    row = lax.broadcasted_iota(jnp.int32, (PANEL, size), 0)
    zero = jnp.zeros((PANEL, size), F32)
    panels = [matrix[i * PANEL : (i + 1) * PANEL] for i in range(count)]

    def spread(panel, column):
        return jnp.broadcast_to(panel[:, column : column + 1], (PANEL, size))

    for i in range(count):
        start = i * PANEL
        inside = (lane >= start) & (lane < start + PANEL)
        panel = panels[i]
        columns = [spread(panel, start + k) for k in range(PANEL)]
        ahead = i + 1 < count
        if ahead:
            next_columns = [spread(panels[i + 1], start + k) for k in range(PANEL)]
        panel = jnp.where(inside, jnp.where(lane - start == row, 1.0, 0.0), panel)
        for k in range(PANEL):
            scale = 1.0 / columns[k][k : k + 1]
            at = row == k
            factor = jnp.where(at, -1.0, columns[k])
            panel = jnp.where(at, 0.0, panel) - factor * (panel[k : k + 1] * scale)
            for j in range(k + 1, PANEL):
                pivot = columns[j][k : k + 1] * scale
                columns[j] = jnp.where(at, 0.0, columns[j]) - factor * pivot
        padded = jnp.concatenate([zero] * i + [panel] + [zero] * (count - 1 - i), 0)
        update = fine(jnp.concatenate(panels, 0), padded, NN)
        if ahead:
            change = next_columns[0] * panel[0:1]
            for k in range(1, PANEL):
                change = change + next_columns[k] * panel[k : k + 1]
        for j in range(count):
            if j == i:
                panels[j] = panel
            else:
                own = update[j * PANEL : (j + 1) * PANEL]
                own = change if j == i + 1 else own
                panels[j] = jnp.where(inside, 0.0, panels[j]) - own
    return jnp.concatenate(panels, 0)


def plan(leaves, groups, levels, rank, rows):
    early = [("c0", rank)]
    late = []
    for j in range(levels):
        height = (levels - j) * rank
        if j == 1:
            early.append(("c1", rank))
        if j < 2:
            height -= rank
        if height:
            (late if j else early).append((f"m{j}", height))
    early.append(("t0", rows))
    if levels > 1:
        late.append(("t1", (levels - 1) * rows))
    return early, late


def other(index, bit):
    return index + bit - 2 * bit * ((index // bit) % 2)


def kernel(cfg, rs_ref, g_ref, b_ref, ord_ref, out_ref, *scratch):
    leaves, groups, levels, rank, own_rows, points, piece = cfg
    rows = groups * own_rows
    early, late = plan(leaves, groups, levels, rank, rows)
    early, late = [name for name, _ in early], [name for name, _ in late]
    names = early + late
    ref = dict(zip(scratch_names(cfg), scratch))
    leaf, position = lax.axis_index("leaf"), lax.axis_index("rhs")
    mesh_id = pl.DeviceIdType.MESH

    def at(leaf_index, rhs_index):
        return {"leaf": leaf_index, "rhs": rhs_index}

    rhs_peers = [lax.rem(position + k, groups) for k in range(1, groups)]
    mate = other(position, 1)
    half = lax.rem(position, 2)
    chips = [(leaf, lax.rem(position + k, groups)) for k in range(2, groups, 2)]
    chips += [(other(leaf, 1), lax.rem(position + k, groups)) for k in range(0, groups, 2)]
    greeted = [(leaf, p) for p in rhs_peers]
    greeted += chips[groups // 2 - 1 :]
    greeted += [(other(leaf, 1 << h), position) for h in range(1, levels)]

    barrier = pltpu.get_barrier_semaphore()
    for target in greeted:
        pl.semaphore_signal(barrier, inc=1, device_id=at(*target), device_id_type=mesh_id)

    def remote(src, dst, sems, slot, target):
        return pltpu.make_async_remote_copy(
            src_ref=src,
            dst_ref=dst,
            send_sem=ref[sems + "_s"].at[slot],
            recv_sem=ref[sems + "_r"].at[slot],
            device_id=at(*target),
            device_id_type=mesh_id,
        )

    g_parts = split(g_ref[...], 3)
    for k, part in enumerate(g_parts):
        ref[f"g{k}"][...] = part
    bases = b_ref[...].reshape(levels * rank, points)
    solved = dot(bases, g_parts[0], NN) + (dot(bases, g_parts[1], NN) + dot(bases, g_parts[2], NN))
    ref["y"][...] = solved
    own_cols = pl.ds(pl.multiple_of(position * piece, piece), piece)
    bases_own = b_ref[:, :, own_cols].reshape(levels * rank, piece)
    gram = sum(dot(part, bases_own, NT) for part in reversed(split(solved, 3)))
    for j in range(levels):
        column = gram[j * rank :, j * rank : (j + 1) * rank]
        if j < 2:
            ref[f"part_c{j}"][...] = column[:rank]
            column = column[rank:]
        if column.shape[0]:
            ref[f"part_m{j}"][...] = column

    pl.semaphore_wait(barrier, len(greeted))

    def halves(buffer, which):
        count = buffer.shape[0] // 2
        return buffer.at[pl.ds(pl.multiple_of(which * count, count), count)]

    def fold_start(name):
        slot = names.index(name)
        copy = remote(
            halves(ref["part_" + name], 1 - half), ref["fold_" + name], "fold", slot, (leaf, mate)
        )
        copy.start()
        return copy

    def spread_start(name, fold):
        fold.wait_recv()
        slot = names.index(name)
        ref["chip_" + name][...] = halves(ref["part_" + name], half)[...] + ref["fold_" + name][...]
        copies = []
        for k, target in enumerate(chips):
            copy = remote(
                ref["chip_" + name],
                ref["peer_" + name].at[k],
                "peer",
                slot * len(chips) + k,
                target,
            )
            copy.start()
            copies.append(copy)
        return copies

    def join_start(name, copies):
        for copy in copies:
            copy.wait_recv()
        total = ref["chip_" + name][...]
        for k in range(len(copies)):
            total = total + ref["peer_" + name][k]
        halves(ref["full_" + name], half)[...] = total
        slot = names.index(name)
        copy = remote(
            halves(ref["full_" + name], half),
            halves(ref["full_" + name], half),
            "join",
            slot,
            (leaf, mate),
        )
        copy.start()
        return copy

    grams = [name for name in names if not name.startswith("t")]
    folds = {name: fold_start(name) for name in grams}

    tile = rank
    order = ord_ref[...]

    def one_hot(i, carry):
        start = pl.multiple_of(i * tile, tile)
        index = lax.broadcasted_iota(jnp.int32, (tile, points), 0) + start
        ref["perm"][pl.ds(start, tile), :] = jnp.where(index == order, 1.0, 0.0).astype(BF16)
        return carry

    lax.fori_loop(0, points // tile, one_hot, 0)
    spreads = {"c0": spread_start("c0", folds["c0"])}
    moved = dot(jnp.concatenate(split(rs_ref[...], 3), 0), ref["perm"][...], NN)
    ref["tree"][...] = (moved[:own_rows] + moved[own_rows : 2 * own_rows]) + moved[2 * own_rows :]
    pieces = []
    for k, peer in enumerate(rhs_peers):
        copy = remote(
            ref["tree"].at[:, pl.ds(pl.multiple_of(peer * piece, piece), piece)],
            ref["cols"].at[position],
            "cols",
            k,
            (leaf, peer),
        )
        copy.start()
        pieces.append(copy)
    ref["cols"][position] = ref["tree"][:, own_cols]
    for name in early[1:]:
        if name in grams:
            spreads[name] = spread_start(name, folds[name])
    for copy in pieces:
        copy.wait_recv()
    term = fine(ref["cols"][...].reshape(rows, piece), ref["y"][...], NT)
    ref["part_t0"][...] = term[:, :rank]
    folds["t0"] = fold_start("t0")
    for j in range(1, levels):
        ref["part_t1"][(j - 1) * rows : j * rows] = term[:, j * rank : (j + 1) * rank]
    if levels > 1:
        folds["t1"] = fold_start("t1")
    spreads["t0"] = spread_start("t0", folds["t0"])
    for name in late:
        spreads[name] = spread_start(name, folds[name])
    sent = []
    for k, peer in enumerate(rhs_peers):
        copy = remote(ref["tree"], ref["rs"].at[position], "rs", k, (leaf, peer))
        copy.start()
        sent.append(copy)
    ref["rs"][position] = ref["tree"][...]

    def plain_term():
        for copy in sent:
            copy.wait_recv()
        gathered = ref["rs"][...].reshape(rows, points)
        stack = jnp.concatenate(split(gathered, 3), 0)
        by_0 = dot(stack, ref["g0"][...], NN)
        by_1 = dot(stack[: 2 * rows], ref["g1"][...], NN)
        by_2 = dot(stack[:rows], ref["g2"][...], NN)
        ref["x"][...] = by_0[:rows] + (
            (by_0[rows : 2 * rows] + by_1[:rows]) + (by_0[2 * rows :] + by_1[rows:] + by_2)
        )

    joins = {"c0": join_start("c0", spreads["c0"])}
    eye = (
        lax.broadcasted_iota(jnp.int32, (rank, rank), 0)
        == lax.broadcasted_iota(jnp.int32, (rank, rank), 1)
    ).astype(F32)
    joins["c0"].wait_recv()

    level_copies = {}
    weights = []
    slots = iter(range(levels * levels * 2))

    def level_start(h, j, which, start, value):
        span = pl.ds(start, value.shape[0])
        ref[f"send{h}_{j}"][span, :] = value
        copy = remote(
            ref[f"send{h}_{j}"].at[span],
            ref[f"get{h}_{j}"].at[span],
            "level",
            next(slots),
            (other(leaf, 1 << h), position),
        )
        copy.start()
        level_copies[h, j, which] = copy

    def level_value(h, j, start):
        return ref[f"send{h}_{j}"][start:] + ref[f"get{h}_{j}"][start:]

    for h in range(levels):
        if h == 0:
            capacity = ref["full_c0"][...]
        else:
            level_copies[h, h, 0].wait_recv()
            capacity = ref[f"send{h}_{h}"][:rank] + ref[f"get{h}_{h}"][:rank]
        inverted = inverse(capacity + eye)
        if h == 0:
            for name in early[1:]:
                joins[name] = join_start(name, spreads[name])
            for name in early[1:]:
                joins[name].wait_recv()
            rest = ref["full_t0"][...]
            if levels > 1:
                rest = jnp.concatenate([ref["full_m0"][...], rest], 0)
                head = ref["full_c1"][...]
        else:
            level_copies[h, h, 1].wait_recv()
            rest = level_value(h, h, rank)
            if h + 1 < levels:
                level_copies[h, h + 1, 1].wait_recv()
                following = level_value(h, h + 1, 0)
                head, tail = following[:rank], following[rank:]
        if h + 1 < levels:
            first = fine(rest[:rank], inverted, NN)
            level_start(h + 1, h + 1, 0, 0, head - fine(first, rest[:rank], NT))
            weight = jnp.concatenate([first, fine(rest[rank:], inverted, NN)], 0)
        else:
            weight = fine(rest, inverted, NN)
        weights.append(weight)
        if h == 0:
            for name in late:
                joins[name] = join_start(name, spreads[name])
            for name in late:
                joins[name].wait_recv()
        for j in range(h + 1, levels):
            offset = (j - h - 1) * rank
            start = rank if j == h + 1 else 0
            if h == 0:
                column = ref["full_t1"][(j - 1) * rows : j * rows]
                if f"m{j}" in names:
                    column = jnp.concatenate([ref[f"full_m{j}"][...], column], 0)
            elif j == h + 1:
                column = tail
            else:
                level_copies[h, j, 1].wait_recv()
                column = level_value(h, j, 0)
            update = fine(weight[offset + start :], rest[offset : offset + rank], NT)
            level_start(h + 1, j, 1, start, column - update)
        if h == max(levels - 2, 0):
            plain_term()

    coefficients = [None] * levels
    for h in reversed(range(levels)):
        value = weights[h][(levels - 1 - h) * rank :]
        for j in range(h + 1, levels):
            offset = (j - h - 1) * rank
            value = value - fine(coefficients[j], weights[h][offset : offset + rank], NN)
        coefficients[h] = value
    answer = ref["x"][...] - fine(jnp.concatenate(coefficients, 1), ref["y"][...], NN)
    ref["answer"][...] = answer.reshape(groups, own_rows, piece)
    last = []
    for k, peer in enumerate(rhs_peers):
        copy = remote(ref["answer"].at[peer], ref["final"].at[position], "last", k, (leaf, peer))
        copy.start()
        last.append(copy)
    ref["final"][position] = ref["answer"][position]
    for copy in last:
        copy.wait_recv()
    tree_rows = jnp.concatenate([ref["final"][k] for k in range(groups)], 1)
    moved = dot(jnp.concatenate(split(tree_rows, 3), 0), ref["perm"][...], NT)
    out_ref[...] = moved[:own_rows] + (moved[own_rows : 2 * own_rows] + moved[2 * own_rows :])

    for copy in pieces + sent + last + list(folds.values()) + list(joins.values()):
        copy.wait_send()
    for copies in spreads.values():
        for copy in copies:
            copy.wait_send()
    for copy in level_copies.values():
        copy.wait_send()


def scratch_list(cfg):
    leaves, groups, levels, rank, own_rows, points, piece = cfg
    rows = groups * own_rows
    early, late = plan(leaves, groups, levels, rank, rows)
    units = early + late
    chips = groups - 1
    items = [
        ("y", pltpu.VMEM((levels * rank, piece), F32)),
        ("x", pltpu.VMEM((rows, piece), F32)),
        ("rs", pltpu.VMEM((groups, own_rows, points), F32)),
        ("tree", pltpu.VMEM((own_rows, points), F32)),
        ("cols", pltpu.VMEM((groups, own_rows, piece), F32)),
        ("g0", pltpu.VMEM((points, piece), BF16)),
        ("g1", pltpu.VMEM((points, piece), BF16)),
        ("g2", pltpu.VMEM((points, piece), BF16)),
        ("perm", pltpu.VMEM((points, points), BF16)),
        ("answer", pltpu.VMEM((groups, own_rows, piece), F32)),
        ("final", pltpu.VMEM((groups, own_rows, piece), F32)),
    ]
    for name, height in units:
        items += [
            ("part_" + name, pltpu.VMEM((height, rank), F32)),
            ("fold_" + name, pltpu.VMEM((height // 2, rank), F32)),
            ("chip_" + name, pltpu.VMEM((height // 2, rank), F32)),
            ("peer_" + name, pltpu.VMEM((chips, height // 2, rank), F32)),
            ("full_" + name, pltpu.VMEM((height, rank), F32)),
        ]
    pairs = 0
    for h in range(1, levels):
        for j in range(h, levels):
            pairs += 1
            height = (levels - j) * rank + rows
            items.append((f"send{h}_{j}", pltpu.VMEM((height, rank), F32)))
            items.append((f"get{h}_{j}", pltpu.VMEM((height, rank), F32)))
    counts = {
        "rs": groups - 1,
        "cols": groups - 1,
        "last": groups - 1,
        "fold": len(units),
        "join": len(units),
        "peer": len(units) * chips,
        "level": max(1, 2 * pairs),
    }
    for name, count in counts.items():
        items.append((name + "_s", pltpu.SemaphoreType.DMA((count,))))
        items.append((name + "_r", pltpu.SemaphoreType.DMA((count,))))
    return items


def scratch_names(cfg):
    return [name for name, _ in scratch_list(cfg)]


def local(right_sides, leaf_inverse, bases, ordering):
    own_rows, points = right_sides.shape
    levels, rank = bases.shape[:2]
    cfg = (
        lax.axis_size("leaf"),
        lax.axis_size("rhs"),
        levels,
        rank,
        own_rows,
        points,
        leaf_inverse.shape[1],
    )
    return pl.pallas_call(
        functools.partial(kernel, cfg),
        out_shape=jax.ShapeDtypeStruct((own_rows, points), F32),
        in_specs=[pl.BlockSpec(memory_space=pltpu.VMEM)] * 4,
        out_specs=pl.BlockSpec(memory_space=pltpu.VMEM),
        scratch_shapes=[item for _, item in scratch_list(cfg)],
        compiler_params=pltpu.CompilerParams(collective_id=0, has_side_effects=True),
        name="tree_solve",
    )(right_sides, leaf_inverse, bases, ordering)


def solution(mesh):
    placed = (P("rhs", "leaf"), P("leaf", "rhs"), P(None, None, "leaf"), P("leaf", None))
    return jax.shard_map(
        local, mesh=mesh, in_specs=placed, out_specs=P("rhs", "leaf"), check_vma=False
    )
```

```python
import functools

import jax
import jax.numpy as jnp
from jax import lax
from jax.experimental import pallas as pl
from jax.experimental.pallas import tpu as pltpu
from jax.sharding import PartitionSpec as P

F32 = jnp.float32
BF16 = jnp.bfloat16
NN = (((1,), (0,)), ((), ()))
NT = (((1,), (1,)), ((), ()))
PANEL = 16


def split(value, pieces):
    parts = []
    for _ in range(pieces):
        head = value.astype(BF16)
        parts.append(head)
        value = value - head.astype(F32)
    return parts


def dot(left, right, dims):
    return lax.dot_general(left, right, dims, preferred_element_type=F32)


def fine(left, right, dims):
    return lax.dot_general(
        left, right, dims, precision=lax.Precision.HIGHEST, preferred_element_type=F32
    )


def inverse(matrix, hooks):
    size = matrix.shape[0]
    count = size // PANEL
    lane = lax.broadcasted_iota(jnp.int32, (PANEL, size), 1)
    row = lax.broadcasted_iota(jnp.int32, (PANEL, size), 0)
    zero = jnp.zeros((PANEL, size), F32)
    panels = [matrix[i * PANEL : (i + 1) * PANEL] for i in range(count)]

    def spread(panel, column):
        return jnp.broadcast_to(panel[:, column : column + 1], (PANEL, size))

    for i in range(count):
        for hook in hooks.get(i, ()):
            hook()
        start = i * PANEL
        inside = (lane >= start) & (lane < start + PANEL)
        panel = panels[i]
        columns = [spread(panel, start + k) for k in range(PANEL)]
        ahead = i + 1 < count
        if ahead:
            next_columns = [spread(panels[i + 1], start + k) for k in range(PANEL)]
        panel = jnp.where(inside, jnp.where(lane - start == row, 1.0, 0.0), panel)
        for k in range(PANEL):
            scale = 1.0 / columns[k][k : k + 1]
            at = row == k
            factor = jnp.where(at, -1.0, columns[k])
            panel = jnp.where(at, 0.0, panel) - factor * (panel[k : k + 1] * scale)
            for j in range(k + 1, PANEL):
                pivot = columns[j][k : k + 1] * scale
                columns[j] = jnp.where(at, 0.0, columns[j]) - factor * pivot
        padded = jnp.concatenate([zero] * i + [panel] + [zero] * (count - 1 - i), 0)
        update = fine(jnp.concatenate(panels, 0), padded, NN)
        if ahead:
            change = next_columns[0] * panel[0:1]
            for k in range(1, PANEL):
                change = change + next_columns[k] * panel[k : k + 1]
        for j in range(count):
            if j == i:
                panels[j] = panel
            else:
                own = update[j * PANEL : (j + 1) * PANEL]
                own = change if j == i + 1 else own
                panels[j] = jnp.where(inside, 0.0, panels[j]) - own
    return jnp.concatenate(panels, 0)


def blocks_of(levels, first):
    later = [(i, first) for i in range(first + 1, levels)]
    for j in range(first + 1, levels):
        later += [(i, j) for i in range(j, levels)]
    return [(first, first)] + later


def direct_units(levels):
    units = {"c": [(0, 0)]}
    if levels > 1:
        units["a"] = [(1, 0), (1, 1)]
    if levels > 2:
        units["d"] = [(i, 0) for i in range(2, levels)]
    return units


def slow_units(levels):
    units = {}
    if levels > 2:
        units["e1"] = [(i, 1) for i in range(2, levels)]
    for j in range(2, levels):
        units[f"e{j}"] = [(i, j) for i in range(j, levels)]
    return units


def bits(count):
    return [1 << k for k in range(count.bit_length() - 1)]


def stages_of(name, groups):
    column = int(name[1:])
    stages = [(2, 0)] + [(0, bit) for bit in bits(groups)[1:]] + [(1, 0)]
    return stages + [(1 << h, 0) for h in range(2, column + 1)]


def other(index, bit):
    return index + bit - 2 * bit * ((index // max(bit, 1)) % 2)


def kernel(cfg, rs_ref, g_ref, b_ref, ord_ref, out_ref, *scratch):
    leaves, groups, levels, rank, own_rows, points, piece = cfg
    rows = groups * own_rows
    ref = dict(zip(scratch_names(cfg), scratch))
    leaf, position = lax.axis_index("leaf"), lax.axis_index("rhs")
    mesh_id = pl.DeviceIdType.MESH
    direct, slow = direct_units(levels), slow_units(levels)

    def at(leaf_index, rhs_index):
        return {"leaf": leaf_index, "rhs": rhs_index}

    rhs_peers = [lax.rem(position + k, groups) for k in range(1, groups)]
    mate = other(position, 1)
    half = lax.rem(position, 2)
    chips = [(leaf, lax.rem(position + k, groups)) for k in range(2, groups, 2)]
    across = [peer for _, peer in chips]
    chips += [(other(leaf, 1), lax.rem(position + k, groups)) for k in range(0, groups, 2)]
    greeted = [(leaf, p) for p in rhs_peers]
    greeted += chips[groups // 2 - 1 :]
    greeted += [(other(leaf, 1 << h), position) for h in range(1, levels)]

    barrier = pltpu.get_barrier_semaphore()
    for target in greeted:
        pl.semaphore_signal(barrier, inc=1, device_id=at(*target), device_id_type=mesh_id)

    started = []

    def send(src, dst, target):
        slot = len(started)
        copy = pltpu.make_async_remote_copy(
            src_ref=src,
            dst_ref=dst,
            send_sem=ref["sent"].at[slot],
            recv_sem=ref["received"].at[slot],
            device_id=at(*target),
            device_id_type=mesh_id,
        )
        copy.start()
        started.append(copy)
        return copy

    def halves(buffer, which):
        count = buffer.shape[0] // 2
        return buffer.at[pl.ds(pl.multiple_of(which * count, count), count)]

    flying = {}

    def fold(name):
        part = halves(ref["part_" + name], 1 - half)
        flying[name] = send(part, ref["fold_" + name], (leaf, mate))

    def folded(name):
        flying[name].wait_recv()
        return halves(ref["part_" + name], half)[...] + ref["fold_" + name][...]

    def join(name, total):
        own = halves(ref["full_" + name], half)
        own[...] = total
        flying[name] = send(own, own, (leaf, mate))

    def scatter(name):
        ref["chip_" + name][...] = folded(name)
        flying[name] = [
            send(ref["chip_" + name], ref["peer_" + name].at[k], target)
            for k, target in enumerate(chips)
        ]

    def gather(name):
        total = ref["chip_" + name][...]
        for k, copy in enumerate(flying[name]):
            copy.wait_recv()
            total = total + ref["peer_" + name][k]
        join(name, total)

    def joined(name):
        flying[name].wait_recv()

    def slow_step(name, stage):
        stages = stages_of(name, groups)
        if stage == 0:
            total = folded(name)
        else:
            flying[name].wait_recv()
            total = ref["pass_" + name][stage - 1] + ref["come_" + name][stage - 1]
        if stage == len(stages):
            join(name, total)
            return
        ref["pass_" + name][stage] = total
        leaf_bit, rhs_bit = stages[stage]
        target = (other(leaf, leaf_bit), other(position, rhs_bit))
        flying[name] = send(ref["pass_" + name].at[stage], ref["come_" + name].at[stage], target)

    todo = {}
    for name in slow:
        count = len(stages_of(name, groups))
        todo[name] = [functools.partial(slow_step, name, k) for k in range(count + 1)]
        todo[name].append(functools.partial(joined, name))

    def step(name, count=1):
        for _ in range(count):
            if todo.get(name):
                todo[name].pop(0)()

    def finish(name):
        while todo.get(name):
            step(name)

    g_parts = split(g_ref[...], 3)
    for k, part in enumerate(g_parts):
        ref[f"g{k}"][...] = part
    own_cols = pl.ds(pl.multiple_of(position * piece, piece), piece)
    bases_own = b_ref[:, :, own_cols].reshape(levels * rank, piece)
    own_y = ref["y"].at[position]

    def gram_of(first, last, width):
        left = b_ref[first:last].reshape((last - first) * rank, points)
        solved = dot(left, g_parts[0], NN) + (
            dot(left, g_parts[1], NN) + dot(left, g_parts[2], NN)
        )
        own_y[first * rank : last * rank] = solved
        right = bases_own[: width * rank]
        return sum(dot(part, right, NT) for part in reversed(split(solved, 3)))

    ref["part_c"][...] = gram_of(0, 1, 1)
    pl.semaphore_wait(barrier, len(greeted))
    fold("c")
    order = ord_ref[...]

    def one_hot(i, carry):
        start = pl.multiple_of(i * rank, rank)
        index = lax.broadcasted_iota(jnp.int32, (rank, points), 0) + start
        ref["perm"][pl.ds(start, rank), :] = jnp.where(index == order, 1.0, 0.0).astype(BF16)
        return carry

    lax.fori_loop(0, points // rank, one_hot, 0)
    moved = dot(jnp.concatenate(split(rs_ref[...], 3), 0), ref["perm"][...], NN)
    tree = (moved[:own_rows] + moved[own_rows : 2 * own_rows]) + moved[2 * own_rows :]
    for k in range(groups):
        ref["tree"][k] = tree[:, k * piece : (k + 1) * piece]
    scatter("c")
    pieces = []
    for peer in rhs_peers:
        pieces.append(send(ref["tree"].at[peer], ref["cols"].at[position], (leaf, peer)))
    ref["cols"][position] = ref["tree"][position]

    def part_store(gram, start, name, blocks):
        for k, (i, j) in enumerate(blocks):
            ref["part_" + name][k * rank : (k + 1) * rank] = gram[
                (i - start) * rank : (i - start + 1) * rank, j * rank : (j + 1) * rank
            ]

    if levels > 1:
        part_store(gram_of(1, 2, 2), 1, "a", direct["a"])
        fold("a")
    if levels > 2:
        gram = gram_of(2, levels, levels)
        later = {name: blocks for name, blocks in direct.items() if name not in "ca"}
        later |= slow
        for name, blocks in later.items():
            part_store(gram, 2, name, blocks)
        scatter("a")
        for name in later:
            fold(name)
    elif levels > 1:
        scatter("a")

    terms = []

    def term_part():
        for copy in pieces:
            copy.wait_recv()
        columns = ref["cols"][...].reshape(rows, piece)
        term = fine(columns, own_y[...], NT)
        for k in range(groups):
            ref["term"][k % 2, k // 2] = term[k * own_rows : (k + 1) * own_rows]
        terms.append(send(ref["term"].at[1 - half], ref["term_fold"], (leaf, mate)))

    def term_cross():
        terms[0].wait_recv()
        ref["term_chip"][...] = ref["term"][half] + ref["term_fold"][...]
        for k, peer in enumerate(across):
            source = ref["term_chip"].at[lax.div(peer, 2)]
            terms.append(send(source, ref["term_get"].at[k], (leaf, peer)))

    def term_sum():
        total = ref["term_chip"][lax.div(position, 2)]
        for k, copy in enumerate(terms[1:]):
            copy.wait_recv()
            total = total + ref["term_get"][k]
        ref["term_pass"][...] = total
        terms.append(send(ref["term_pass"], ref["term_come"], (other(leaf, 1), position)))

    def term_joined():
        terms[-1].wait_recv()

    plain = []

    def plain_part():
        stack = jnp.concatenate(split(ref["cols"][...].reshape(rows, piece), 3), 0)
        by_0 = dot(stack, ref["g0"][...], NT)
        by_1 = dot(stack[: 2 * rows], ref["g1"][...], NT)
        by_2 = dot(stack[:rows], ref["g2"][...], NT)
        value = by_0[:rows] + (
            (by_0[rows : 2 * rows] + by_1[:rows]) + (by_0[2 * rows :] + by_1[rows:] + by_2)
        )
        for k in range(groups):
            ref["plain"][k % 2, k // 2] = value[k * own_rows : (k + 1) * own_rows]
        plain.append(send(ref["plain"].at[1 - half], ref["plain_fold"], (leaf, mate)))

    def plain_cross():
        plain[0].wait_recv()
        ref["plain_chip"][...] = ref["plain"][half] + ref["plain_fold"][...]
        for k, peer in enumerate(across):
            source = ref["plain_chip"].at[lax.div(peer, 2)]
            plain.append(send(source, ref["plain_get"].at[k], (leaf, peer)))

    def plain_sum():
        total = ref["plain_chip"][lax.div(position, 2)]
        for k, copy in enumerate(plain[1:]):
            copy.wait_recv()
            total = total + ref["plain_get"][k]
        ref["x"][...] = total

    solved_copies, relays = [], []

    def solved_send():
        for peer in across:
            solved_copies.append(send(own_y, own_y, (leaf, peer)))
        relays.append(send(own_y, own_y, (leaf, mate)))

    def solved_relay():
        for k, copy in enumerate(solved_copies):
            copy.wait_recv()
            source = lax.rem(position + groups - 2 * (k + 1), groups)
            slot = ref["y"].at[source]
            relays.append(send(slot, slot, (leaf, mate)))

    def solved_done():
        for copy in relays:
            copy.wait_recv()
        for k in range(groups):
            for p, part in enumerate(split(ref["y"][k], 2)):
                ref[f"y{p}"][:, k * piece : (k + 1) * piece] = part

    eye = (
        lax.broadcasted_iota(jnp.int32, (rank, rank), 0)
        == lax.broadcasted_iota(jnp.int32, (rank, rank), 1)
    ).astype(F32)
    linear = {}
    for name, blocks in [*direct.items(), *slow.items()]:
        for k, block in enumerate(blocks):
            linear[block] = (name, k * rank)
    place = {}
    for h in range(1, levels):
        for k, block in enumerate(blocks_of(levels, h)):
            place[h, block] = k * rank

    def linear_value(block):
        name, start = linear[block]
        return ref["full_" + name][start : start + rank]

    def carried(h, block):
        start = place[h, block]
        span = slice(start, start + rank)
        return ref[f"send{h}"][span] + ref[f"get{h}"][span]

    def block_value(h, block):
        if h == 0:
            return linear_value(block)
        value = carried(h, block)
        return value if block == (1, 1) else value + linear_value(block)

    def term_value(h, j):
        if h == 0:
            span = slice(j * rank, (j + 1) * rank)
            return ref["term_pass"][:, span] + ref["term_come"][:, span]
        start = (j - h) * own_rows
        span = slice(start, start + own_rows)
        return ref[f"tsend{h}"][span] + ref[f"tget{h}"][span]

    level_copies = {}

    def level_send(h, part, start, stop):
        span = pl.ds(start, stop - start)
        level_copies[h, part] = send(
            ref[f"send{h}"].at[span], ref[f"get{h}"].at[span], (other(leaf, 1 << h), position)
        )

    def level_wait(h, part):
        copy = level_copies.pop((h, part), None)
        if copy is not None:
            copy.wait_recv()

    inverses = [None] * levels
    below = [None] * levels
    weights = {}
    term_weights = {}

    def level_terms(h):
        if h:
            level_wait(h, "terms")
        term_weights[h] = fine(term_value(h, h), inverses[h], NN)
        if h + 1 < levels:
            for k, j in enumerate(range(h + 1, levels)):
                change = fine(term_weights[h], below[h][j], NT)
                span = slice(k * own_rows, (k + 1) * own_rows)
                ref[f"tsend{h + 1}"][span] = term_value(h, j) - change
            level_copies[h + 1, "terms"] = send(
                ref[f"tsend{h + 1}"], ref[f"tget{h + 1}"], (other(leaf, 2 << h), position)
            )

    def level_change(h, block):
        i, j = block
        change = fine(weights[i, h], below[h][j], NT)
        if block == (1, 1):
            return linear_value(block) - change
        return carried(h, block) - change if h else -change

    def level_body(h):
        level_wait(h, "rest")
        target = ref[f"send{h + 1}"]
        blocks = blocks_of(levels, h + 1)
        split_at = levels - h - 1
        for part, first, last in (("column", 1, split_at), ("rest", split_at, len(blocks))):
            for k in range(first, last):
                target[k * rank : (k + 1) * rank] = level_change(h, blocks[k])
            if last > first:
                level_send(h + 1, part, first * rank, last * rank)

    for name in slow:
        step(name)
    gather("c")
    term_part()
    joined("c")
    hooks = {h: {} for h in range(levels)}
    hooks[0] = {
        1: [lambda: scatter("d")] if "d" in direct else [],
        2: [term_cross],
        4: [lambda: step("e1"), lambda: step("e2")],
        6: [lambda: gather("a")] if "a" in direct else [],
    }
    if levels > 2:
        hooks[1] = {
            3: [lambda: step("e1"), lambda: step("e2")],
            5: [term_joined, lambda: level_terms(0)],
            7: [lambda: finish("e1")],
        }
    for h in range(2, levels):
        hooks[h] = {}
    for h in range(levels):
        if h:
            level_wait(h, "head")
            if h > 1:
                finish(f"e{h}")
        inverses[h] = inverse(block_value(h, (h, h)) + eye, hooks[h])
        if h + 1 == levels:
            break
        if h == 0:
            joined("a")
        else:
            level_wait(h, "column")
            finish(f"e{h}")
        first = block_value(h, (h + 1, h))
        below[h] = {h + 1: first}
        weights[h + 1, h] = fine(first, inverses[h], NN)
        if h:
            level_wait(h, "rest")
        ref[f"send{h + 1}"][:rank] = level_change(h, (h + 1, h + 1))
        level_send(h + 1, "head", 0, rank)
        if h + 2 < levels:
            if h == 0:
                gather("d")
                step("e1")
                step("e2")
                joined("d")
            for i in range(h + 2, levels):
                below[h][i] = block_value(h, (i, h))
                weights[i, h] = fine(below[h][i], inverses[h], NN)
            level_body(h)
        if h == 0:
            term_sum()
            solved_send()
            plain_part()
        if h == levels - 2:
            if h == 0:
                term_joined()
                level_terms(0)
            step("e2")
        if h:
            level_terms(h)
        if h == levels - 2:
            hooks[h + 1] |= {0: [plain_cross], 1: [solved_relay], 6: [solved_done], 7: [plain_sum]}
    if levels == 1:
        term_sum()
        solved_send()
        plain_part()
        term_joined()
        plain_cross()
        solved_relay()
        plain_sum()
        solved_done()
    level_terms(levels - 1)

    coefficients = [None] * levels
    for h in reversed(range(levels)):
        value = term_weights[h]
        for j in range(h + 1, levels):
            value = value - fine(coefficients[j], weights[j, h], NN)
        coefficients[h] = value
    stack = jnp.concatenate(split(jnp.concatenate(coefficients, 1), 2), 0)
    by_0 = dot(stack, ref["y0"][...], NN)
    by_1 = dot(stack[:own_rows], ref["y1"][...], NN)
    tree_rows = ref["x"][...] - (by_0[:own_rows] + (by_0[own_rows:] + by_1))
    moved = dot(jnp.concatenate(split(tree_rows, 3), 0), ref["perm"][...], NT)
    out_ref[...] = moved[:own_rows] + (moved[own_rows : 2 * own_rows] + moved[2 * own_rows :])

    for copy in started:
        copy.wait_send()


def scratch_list(cfg):
    leaves, groups, levels, rank, own_rows, points, piece = cfg
    chips = groups - 1
    width = levels * rank
    direct, slow = direct_units(levels), slow_units(levels)
    items = [
        ("y", pltpu.VMEM((groups, width, piece), F32)),
        ("y0", pltpu.VMEM((width, points), BF16)),
        ("y1", pltpu.VMEM((width, points), BF16)),
        ("x", pltpu.VMEM((own_rows, points), F32)),
        ("tree", pltpu.VMEM((groups, own_rows, piece), F32)),
        ("cols", pltpu.VMEM((groups, own_rows, piece), F32)),
        ("plain", pltpu.VMEM((2, groups // 2, own_rows, points), F32)),
        ("plain_fold", pltpu.VMEM((groups // 2, own_rows, points), F32)),
        ("plain_chip", pltpu.VMEM((groups // 2, own_rows, points), F32)),
        ("plain_get", pltpu.VMEM((max(1, groups // 2 - 1), own_rows, points), F32)),
        ("term", pltpu.VMEM((2, groups // 2, own_rows, width), F32)),
        ("term_fold", pltpu.VMEM((groups // 2, own_rows, width), F32)),
        ("term_chip", pltpu.VMEM((groups // 2, own_rows, width), F32)),
        ("term_get", pltpu.VMEM((max(1, groups // 2 - 1), own_rows, width), F32)),
        ("term_pass", pltpu.VMEM((own_rows, width), F32)),
        ("term_come", pltpu.VMEM((own_rows, width), F32)),
        ("g0", pltpu.VMEM((points, piece), BF16)),
        ("g1", pltpu.VMEM((points, piece), BF16)),
        ("g2", pltpu.VMEM((points, piece), BF16)),
        ("perm", pltpu.VMEM((points, points), BF16)),
    ]
    count = 3 * groups + 4 * (levels - 1)
    for name, blocks in [*direct.items(), *slow.items()]:
        height = len(blocks) * rank
        items += [
            ("part_" + name, pltpu.VMEM((height, rank), F32)),
            ("fold_" + name, pltpu.VMEM((height // 2, rank), F32)),
            ("full_" + name, pltpu.VMEM((height, rank), F32)),
        ]
        if name in direct:
            count += 2 + chips
            items += [
                ("chip_" + name, pltpu.VMEM((height // 2, rank), F32)),
                ("peer_" + name, pltpu.VMEM((chips, height // 2, rank), F32)),
            ]
        else:
            stages = len(stages_of(name, groups))
            count += 2 + stages
            items += [
                ("pass_" + name, pltpu.VMEM((stages, height // 2, rank), F32)),
                ("come_" + name, pltpu.VMEM((stages, height // 2, rank), F32)),
            ]
    for h in range(1, levels):
        height = len(blocks_of(levels, h)) * rank
        items.append((f"send{h}", pltpu.VMEM((height, rank), F32)))
        items.append((f"get{h}", pltpu.VMEM((height, rank), F32)))
        height = (levels - h) * own_rows
        items.append((f"tsend{h}", pltpu.VMEM((height, rank), F32)))
        items.append((f"tget{h}", pltpu.VMEM((height, rank), F32)))
    items.append(("sent", pltpu.SemaphoreType.DMA((count,))))
    items.append(("received", pltpu.SemaphoreType.DMA((count,))))
    return items


def scratch_names(cfg):
    return [name for name, _ in scratch_list(cfg)]


def local(right_sides, leaf_inverse, bases, ordering):
    own_rows, points = right_sides.shape
    levels, rank = bases.shape[:2]
    cfg = (
        lax.axis_size("leaf"),
        lax.axis_size("rhs"),
        levels,
        rank,
        own_rows,
        points,
        leaf_inverse.shape[1],
    )
    return pl.pallas_call(
        functools.partial(kernel, cfg),
        out_shape=jax.ShapeDtypeStruct((own_rows, points), F32),
        in_specs=[pl.BlockSpec(memory_space=pltpu.VMEM)] * 4,
        out_specs=pl.BlockSpec(memory_space=pltpu.VMEM),
        scratch_shapes=[item for _, item in scratch_list(cfg)],
        compiler_params=pltpu.CompilerParams(collective_id=0, has_side_effects=True),
        name="tree_solve",
    )(right_sides, leaf_inverse, bases, ordering)


def solution(mesh):
    placed = (P("rhs", "leaf"), P("leaf", "rhs"), P(None, None, "leaf"), P("leaf", None))
    return jax.shard_map(
        local, mesh=mesh, in_specs=placed, out_specs=P("rhs", "leaf"), check_vma=False
    )
```

```python
import functools
import itertools

import jax
import jax.numpy as jnp
from jax import lax
from jax.experimental import pallas as pl
from jax.experimental.pallas import tpu as pltpu
from jax.sharding import PartitionSpec as P

F32 = jnp.float32
BF16 = jnp.bfloat16
NN = (((1,), (0,)), ((), ()))
NT = (((1,), (1,)), ((), ()))
PANEL = 16
CHUNKS = 4
POOL = 12


def split(value, pieces):
    parts = []
    for _ in range(pieces):
        head = value.astype(BF16)
        parts.append(head)
        value = value - head.astype(F32)
    return parts


def dot(left, right, dims):
    return lax.dot_general(left, right, dims, preferred_element_type=F32)


def fine(left, right, dims):
    return lax.dot_general(
        left, right, dims, precision=lax.Precision.HIGHEST, preferred_element_type=F32
    )


def inverse(matrix, hooks):
    size = matrix.shape[0]
    count = size // PANEL
    lane = lax.broadcasted_iota(jnp.int32, (PANEL, size), 1)
    row = lax.broadcasted_iota(jnp.int32, (PANEL, size), 0)
    zero = jnp.zeros((PANEL, size), F32)
    panels = [matrix[i * PANEL : (i + 1) * PANEL] for i in range(count)]

    def spread(panel, column):
        return jnp.broadcast_to(panel[:, column : column + 1], (PANEL, size))

    for i in range(count):
        for hook in hooks.get(i, ()):
            hook()
        start = i * PANEL
        inside = (lane >= start) & (lane < start + PANEL)
        panel = panels[i]
        columns = [spread(panel, start + k) for k in range(PANEL)]
        ahead = i + 1 < count
        if ahead:
            next_columns = [spread(panels[i + 1], start + k) for k in range(PANEL)]
        panel = jnp.where(inside, jnp.where(lane - start == row, 1.0, 0.0), panel)
        for k in range(PANEL):
            scale = 1.0 / columns[k][k : k + 1]
            at = row == k
            factor = jnp.where(at, -1.0, columns[k])
            panel = jnp.where(at, 0.0, panel) - factor * (panel[k : k + 1] * scale)
            for j in range(k + 1, PANEL):
                pivot = columns[j][k : k + 1] * scale
                columns[j] = jnp.where(at, 0.0, columns[j]) - factor * pivot
        padded = jnp.concatenate([zero] * i + [panel] + [zero] * (count - 1 - i), 0)
        update = fine(jnp.concatenate(panels, 0), padded, NN)
        if ahead:
            change = next_columns[0] * panel[0:1]
            for k in range(1, PANEL):
                change = change + next_columns[k] * panel[k : k + 1]
        for j in range(count):
            if j == i:
                panels[j] = panel
            else:
                own = update[j * PANEL : (j + 1) * PANEL]
                own = change if j == i + 1 else own
                panels[j] = jnp.where(inside, 0.0, panels[j]) - own
    return jnp.concatenate(panels, 0)


def blocks_of(levels, first):
    later = [(i, first) for i in range(first + 1, levels)]
    for j in range(first + 1, levels):
        later += [(i, j) for i in range(j, levels)]
    return [(first, first)] + later


def direct_units(levels):
    units = {"c": [(0, 0)]}
    if levels > 1:
        units["a"] = [(1, 0), (1, 1)]
    if levels > 2:
        units["d"] = [(i, 0) for i in range(2, levels)]
    return units


def slow_units(levels):
    units = {}
    if levels > 2:
        units["e1"] = [(i, 1) for i in range(2, levels)]
    for j in range(2, levels):
        units[f"e{j}"] = [(i, j) for i in range(j, levels)]
    return units


def stages_of(name):
    column = int(name[1:])
    return [1 << h for h in range(1, column + 1)] + [None]


def other(index, bit):
    return index + bit - 2 * bit * ((index // max(bit, 1)) % 2)


def kernel(cfg, rs_hbm, g_hbm, b_hbm, ord_hbm, out_ref, *scratch):
    leaves, groups, levels, rank, own_rows, points, piece = cfg
    rows = groups * own_rows
    ref = dict(zip(scratch_names(cfg), scratch))
    leaf, position = lax.axis_index("leaf"), lax.axis_index("rhs")
    mesh_id = pl.DeviceIdType.MESH
    direct, slow = direct_units(levels), slow_units(levels)

    def at(leaf_index, rhs_index):
        return {"leaf": leaf_index, "rhs": rhs_index}

    rhs_peers = [lax.rem(position + k, groups) for k in range(1, groups)]
    mate = other(position, 1)
    half = lax.rem(position, 2)
    chips = [(leaf, lax.rem(position + k, groups)) for k in range(2, groups, 2)]
    across = [peer for _, peer in chips]
    chips += [(other(leaf, 1), lax.rem(position + k, groups)) for k in range(0, groups, 2)]
    greeted = [(leaf, p) for p in rhs_peers]
    greeted += chips[groups // 2 - 1 :]
    greeted += [(other(leaf, 1 << h), position) for h in range(1, levels)]

    rs_ref, g_ref, b_ref, ord_ref = (ref[name] for name in ("rs", "g", "b", "ord"))
    chunk = points // CHUNKS
    moves = [(b_hbm.at[0], b_ref.at[0])]
    for k in range(CHUNKS):
        span = pl.ds(k * chunk, chunk)
        moves.append((g_hbm.at[span], g_ref.at[span]))
    moves += [(ord_hbm, ord_ref), (rs_hbm, rs_ref)]
    if levels > 1:
        later = pl.ds(1, levels - 1)
        moves.append((b_hbm.at[later], b_ref.at[later]))
    loads = [
        pltpu.make_async_copy(src, dst, ref["sent"].at[POOL - 1 - k]) for k, (src, dst) in enumerate(moves)
    ]
    urgent = CHUNKS + 1
    for load in loads[:urgent]:
        load.start()
    barrier = pltpu.get_barrier_semaphore()
    for target in greeted:
        pl.semaphore_signal(barrier, inc=1, device_id=at(*target), device_id_type=mesh_id)

    pool = {}
    turn = itertools.count()
    slots = itertools.count()

    def start(src, dst, target, receive, place):
        if place in pool:
            pool[place].wait_send()
        copy = pltpu.make_async_remote_copy(
            src_ref=src,
            dst_ref=dst,
            send_sem=ref["sent"].at[place],
            recv_sem=ref["received"].at[receive],
            device_id=at(*target),
            device_id_type=mesh_id,
        )
        copy.start()
        pool[place] = copy
        return copy

    def send(src, dst, target):
        return start(src, dst, target, next(slots), next(turn) % POOL)

    class Group:
        def __init__(self, copies, landed):
            receive = next(slots)
            for src, dst, target in copies:
                start(src, dst, target, receive, next(turn) % POOL)
            self.wait = pltpu.make_async_copy(landed, landed, ref["received"].at[receive])

        def wait_recv(self):
            self.wait.wait()

    def halves(buffer, which):
        count = buffer.shape[0] // 2
        return buffer.at[pl.ds(pl.multiple_of(which * count, count), count)]

    flying = {}

    def fold(name):
        part = halves(ref["part_" + name], 1 - half)
        flying[name] = send(part, ref["fold_" + name], (leaf, mate))

    def folded(name):
        flying[name].wait_recv()
        return halves(ref["part_" + name], half)[...] + ref["fold_" + name][...]

    def join(name, total):
        own = halves(ref["full_" + name], half)
        own[...] = total
        flying[name] = send(own, own, (leaf, mate))

    def scatter(name):
        ref["chip_" + name][...] = folded(name)
        peers = ref["peer_" + name]
        copies = [(ref["chip_" + name], peers.at[k], target) for k, target in enumerate(chips)]
        flying[name] = Group(copies, peers)

    def gather(name):
        total = ref["chip_" + name][...]
        flying[name].wait_recv()
        for k in range(len(chips)):
            total = total + ref["peer_" + name][k]
        join(name, total)

    def joined(name):
        flying[name].wait_recv()

    def slow_step(name, stage):
        stages = stages_of(name)
        if stage == 0:
            total = folded(name)
        else:
            total = ref["pass_" + name][stage - 1]
            flying[name].wait_recv()
            for k in range(1 if stages[stage - 1] else len(chips)):
                total = total + ref["come_" + name][stage - 1 + k]
        if stage == len(stages):
            join(name, total)
            return
        ref["pass_" + name][stage] = total
        if stages[stage] is None:
            targets = chips
        else:
            targets = [(other(leaf, stages[stage]), position)]
        own, landed = ref["pass_" + name].at[stage], ref["come_" + name]
        copies = [(own, landed.at[stage + k], target) for k, target in enumerate(targets)]
        flying[name] = Group(copies, landed.at[pl.ds(stage, len(targets))])

    todo = {}
    for name in slow:
        count = len(stages_of(name))
        todo[name] = [functools.partial(slow_step, name, k) for k in range(count + 1)]
        todo[name].append(functools.partial(joined, name))

    def step(name, count=1):
        for _ in range(count):
            if todo.get(name):
                todo[name].pop(0)()

    def finish(name):
        while todo.get(name):
            step(name)

    own_cols = pl.ds(pl.multiple_of(position * piece, piece), piece)
    own_y = ref["y"].at[position]

    def products(left, parts):
        return dot(left, parts[0], NN) + (dot(left, parts[1], NN) + dot(left, parts[2], NN))

    def gram_of(solved, first, width):
        own_y[first * rank : first * rank + solved.shape[0]] = solved
        right = b_ref[:width, :, own_cols].reshape(width * rank, piece)
        return sum(dot(part, right, NT) for part in reversed(split(solved, 3)))

    def solved_of(first, last):
        left = b_ref[first:last].reshape((last - first) * rank, points)
        return products(left, [ref[f"g{k}"][...] for k in range(3)])

    loads[0].wait()
    solved = None
    for c in range(CHUNKS):
        loads[1 + c].wait()
        if c == 1:
            for load in loads[urgent:]:
                load.start()
        span = slice(c * chunk, (c + 1) * chunk)
        parts = split(g_ref[span], 3)
        for k, part in enumerate(parts):
            ref[f"g{k}"][span] = part
        value = products(b_ref[0, :, span], parts)
        solved = value if c == 0 else solved + value
    ref["part_c"][...] = gram_of(solved, 0, 1)
    pl.semaphore_wait(barrier, len(greeted))
    fold("c")
    for load in loads[urgent : urgent + 2]:
        load.wait()
    order = ord_ref[...]

    def one_hot(i, carry):
        start = pl.multiple_of(i * rank, rank)
        index = lax.broadcasted_iota(jnp.int32, (rank, points), 0) + start
        ref["perm"][pl.ds(start, rank), :] = jnp.where(index == order, 1.0, 0.0).astype(BF16)
        return carry

    lax.fori_loop(0, points // rank, one_hot, 0)
    moved = dot(jnp.concatenate(split(rs_ref[...], 3), 0), ref["perm"][...], NN)
    tree = (moved[:own_rows] + moved[own_rows : 2 * own_rows]) + moved[2 * own_rows :]
    for k in range(groups):
        ref["tree"][k] = tree[:, k * piece : (k + 1) * piece]
    scatter("c")
    def part_store(gram, start, name, blocks):
        for k, (i, j) in enumerate(blocks):
            ref["part_" + name][k * rank : (k + 1) * rank] = gram[
                (i - start) * rank : (i - start + 1) * rank, j * rank : (j + 1) * rank
            ]

    if levels > 1:
        loads[urgent + 2].wait()
        part_store(gram_of(solved_of(1, 2), 1, 2), 1, "a", direct["a"])
        fold("a")
    ref["cols"][position] = ref["tree"][position]
    copies = [
        (ref["tree"].at[peer], ref["cols_get"].at[k], (leaf, peer))
        for k, peer in enumerate(rhs_peers)
    ]
    pieces = Group(copies, ref["cols_get"])
    if levels > 2:
        gram = gram_of(solved_of(2, levels), 2, levels)
        later = {name: blocks for name, blocks in direct.items() if name not in "ca"}
        later |= slow
        for name, blocks in later.items():
            part_store(gram, 2, name, blocks)
        scatter("a")
        for name in later:
            fold(name)
    elif levels > 1:
        scatter("a")

    terms = []

    def term_part():
        pieces.wait_recv()
        for k in range(groups - 1):
            source = lax.rem(position + groups - 1 - k, groups)
            ref["cols"][source] = ref["cols_get"][k]
        columns = ref["cols"][...].reshape(rows, piece)
        term = fine(columns, own_y[...], NT)
        for k in range(groups):
            ref["term"][k % 2, k // 2] = term[k * own_rows : (k + 1) * own_rows]
        terms.append(send(ref["term"].at[1 - half], ref["term_fold"], (leaf, mate)))

    def term_cross():
        terms[0].wait_recv()
        ref["term_chip"][...] = ref["term"][half] + ref["term_fold"][...]
        for k, peer in enumerate(across):
            source = ref["term_chip"].at[lax.div(peer, 2)]
            terms.append(send(source, ref["term_get"].at[k], (leaf, peer)))

    def term_sum():
        total = ref["term_chip"][lax.div(position, 2)]
        for k, copy in enumerate(terms[1:]):
            copy.wait_recv()
            total = total + ref["term_get"][k]
        ref["term_pass"][...] = total
        terms.append(send(ref["term_pass"], ref["term_come"], (other(leaf, 1), position)))

    def term_joined():
        terms[-1].wait_recv()

    plain = []

    def plain_part():
        stack = jnp.concatenate(split(ref["cols"][...].reshape(rows, piece), 3), 0)
        by_0 = dot(stack, ref["g0"][...], NT)
        by_1 = dot(stack[: 2 * rows], ref["g1"][...], NT)
        by_2 = dot(stack[:rows], ref["g2"][...], NT)
        value = by_0[:rows] + (
            (by_0[rows : 2 * rows] + by_1[:rows]) + (by_0[2 * rows :] + by_1[rows:] + by_2)
        )
        for k in range(groups):
            ref["plain"][k % 2, k // 2] = value[k * own_rows : (k + 1) * own_rows]
        plain.append(send(ref["plain"].at[1 - half], ref["plain_fold"], (leaf, mate)))

    def plain_cross():
        plain[0].wait_recv()
        ref["plain_chip"][...] = ref["plain"][half] + ref["plain_fold"][...]
        for k, peer in enumerate(across):
            source = ref["plain_chip"].at[lax.div(peer, 2)]
            plain.append(send(source, ref["plain_get"].at[k], (leaf, peer)))

    def plain_sum():
        total = ref["plain_chip"][lax.div(position, 2)]
        for k, copy in enumerate(plain[1:]):
            copy.wait_recv()
            total = total + ref["plain_get"][k]
        ref["x"][...] = total

    solved_copies, relays = [], []

    def solved_across(first, last, place):
        part = own_y.at[pl.ds(first * rank, (last - first) * rank)]
        for k, peer in enumerate(across):
            solved_copies.append(start(part, part, (leaf, peer), next(slots), place + k))

    def solved_send(part):
        early = 1
        if part == 0:
            solved_across(0, early, POOL)
        else:
            if early < levels:
                solved_across(early, levels, POOL + len(across))
            place = POOL + 2 * len(across)
            relays.append(start(own_y, own_y, (leaf, mate), next(slots), place))

    def solved_relay():
        for copy in solved_copies:
            copy.wait_recv()
        for k in range(len(across)):
            source = lax.rem(position + groups - 2 * (k + 1), groups)
            slot = ref["y"].at[source]
            place = POOL + 2 * len(across) + 1 + k
            relays.append(start(slot, slot, (leaf, mate), next(slots), place))

    def solved_done():
        for copy in relays:
            copy.wait_recv()
        for k in range(groups):
            for p, part in enumerate(split(ref["y"][k], 2)):
                ref[f"y{p}"][:, k * piece : (k + 1) * piece] = part

    eye = (
        lax.broadcasted_iota(jnp.int32, (rank, rank), 0)
        == lax.broadcasted_iota(jnp.int32, (rank, rank), 1)
    ).astype(F32)
    linear = {}
    for name, blocks in [*direct.items(), *slow.items()]:
        for k, block in enumerate(blocks):
            linear[block] = (name, k * rank)
    place = {}
    for h in range(1, levels):
        for k, block in enumerate(blocks_of(levels, h)):
            place[h, block] = k * rank

    def linear_value(block):
        name, start = linear[block]
        return ref["full_" + name][start : start + rank]

    def carried(h, block):
        start = place[h, block]
        span = slice(start, start + rank)
        return ref[f"send{h}"][span] + ref[f"get{h}"][span]

    def block_value(h, block):
        if h == 0:
            return linear_value(block)
        value = carried(h, block)
        return value if block == (1, 1) else value + linear_value(block)

    def term_value(h, j):
        if h == 0:
            span = slice(j * rank, (j + 1) * rank)
            return ref["term_pass"][:, span] + ref["term_come"][:, span]
        start = (j - h) * own_rows
        span = slice(start, start + own_rows)
        return ref[f"tsend{h}"][span] + ref[f"tget{h}"][span]

    level_copies = {}

    def level_send(h, part, start, stop):
        span = pl.ds(start, stop - start)
        level_copies[h, part] = send(
            ref[f"send{h}"].at[span], ref[f"get{h}"].at[span], (other(leaf, 1 << h), position)
        )

    def level_wait(h, part):
        copy = level_copies.pop((h, part), None)
        if copy is not None:
            copy.wait_recv()

    inverses = [None] * levels
    below = [None] * levels
    weights = {}
    term_weights = {}

    def level_terms(h):
        if h:
            level_wait(h, "terms")
        term_weights[h] = fine(term_value(h, h), inverses[h], NN)
        if h + 1 < levels:
            for k, j in enumerate(range(h + 1, levels)):
                change = fine(term_weights[h], below[h][j], NT)
                span = slice(k * own_rows, (k + 1) * own_rows)
                ref[f"tsend{h + 1}"][span] = term_value(h, j) - change

    def terms_send(h):
        level_copies[h + 1, "terms"] = send(
            ref[f"tsend{h + 1}"], ref[f"tget{h + 1}"], (other(leaf, 2 << h), position)
        )

    def level_change(h, block):
        i, j = block
        change = fine(weights[i, h], below[h][j], NT)
        if block == (1, 1):
            return linear_value(block) - change
        return carried(h, block) - change if h else -change

    def level_body(h):
        level_wait(h, "rest")
        target = ref[f"send{h + 1}"]
        blocks = blocks_of(levels, h + 1)
        split_at = levels - h - 1
        for part, first, last in (("column", 1, split_at), ("rest", split_at, len(blocks))):
            for k in range(first, last):
                target[k * rank : (k + 1) * rank] = level_change(h, blocks[k])
            if last > first:
                level_send(h + 1, part, first * rank, last * rank)

    for name in slow:
        step(name)
    gather("c")
    term_part()
    joined("c")
    hooks = {h: {} for h in range(levels)}
    if levels > 1:
        hooks[0] = {5: [lambda: gather("a")]}
    if levels > 2:
        hooks[0][1] = [lambda: scatter("d")]
        hooks[0][3] = [term_cross]
        hooks[0][4] = [lambda: step("e1"), lambda: step("e2")]
        hooks[1] = {
            5: [lambda: step("e1")],
            6: [term_joined, lambda: level_terms(0)],
            7: [lambda: terms_send(0)],
        }
    else:
        hooks[0][2] = [term_cross]
    carry, partial = [None] * levels, [None] * levels
    for h in range(levels):
        last = h == levels - 1
        if h:
            level_wait(h, "head")
            if h > 1:
                finish(f"e{h}")
        if last:
            if h == 0:
                term_sum()
                solved_send(0)
                solved_send(1)
                plain_part()
                plain_cross()
                term_joined()
            hooks[h] |= {1: [solved_relay], 5: [solved_done]}
        inverses[h] = inverse(block_value(h, (h, h)) + eye, hooks[h])
        if last:
            break
        if h == 0:
            joined("a")
        else:
            level_wait(h, "column")
            finish(f"e{h}")
        first = block_value(h, (h + 1, h))
        below[h] = {h + 1: first}
        weights[h + 1, h] = fine(first, inverses[h], NN)
        if h:
            level_wait(h, "rest")
        ref[f"send{h + 1}"][:rank] = level_change(h, (h + 1, h + 1))
        level_send(h + 1, "head", 0, rank)
        if h + 2 < levels:
            if h == 0:
                solved_send(0)
                gather("d")
                plain_part()
                joined("d")
            for i in range(h + 2, levels):
                below[h][i] = block_value(h, (i, h))
                weights[i, h] = fine(below[h][i], inverses[h], NN)
            level_body(h)
        if h == 0:
            term_sum()
            step("e2")
            if levels == 2:
                solved_send(0)
            solved_send(1)
            if levels == 2:
                plain_part()
        if h or levels == 2:
            if h == 0:
                term_joined()
            if h == levels - 2:
                step("e2")
                plain_cross()
            level_terms(h)
            terms_send(h)
        if h == levels - 2:
            for k in reversed(range(levels - 1)):
                carry[k] = weights[levels - 1, k]
                partial[k] = term_weights[k]
                for j in range(k + 1, levels - 1):
                    carry[k] = carry[k] - fine(carry[j], weights[j, k], NN)
                    partial[k] = partial[k] - fine(partial[j], weights[j, k], NN)
    level_terms(levels - 1)
    plain_sum()

    coefficients = [term_weights[levels - 1] if h == levels - 1 else partial[h] for h in range(levels)]
    for h in range(levels - 1):
        coefficients[h] = coefficients[h] - fine(coefficients[levels - 1], carry[h], NN)
    stack = jnp.concatenate(split(jnp.concatenate(coefficients, 1), 2), 0)
    by_0 = dot(stack, ref["y0"][...], NN)
    by_1 = dot(stack[:own_rows], ref["y1"][...], NN)
    tree_rows = ref["x"][...] - (by_0[:own_rows] + (by_0[own_rows:] + by_1))
    moved = dot(jnp.concatenate(split(tree_rows, 3), 0), ref["perm"][...], NT)
    out_ref[...] = moved[:own_rows] + (moved[own_rows : 2 * own_rows] + moved[2 * own_rows :])

    for copy in pool.values():
        copy.wait_send()


def scratch_list(cfg):
    leaves, groups, levels, rank, own_rows, points, piece = cfg
    chips = groups - 1
    width = levels * rank
    direct, slow = direct_units(levels), slow_units(levels)
    items = [
        ("rs", pltpu.VMEM((own_rows, points), F32)),
        ("g", pltpu.VMEM((points, piece), F32)),
        ("b", pltpu.VMEM((levels, rank, points), BF16)),
        ("ord", pltpu.VMEM((1, points), jnp.int32)),
        ("y", pltpu.VMEM((groups, width, piece), F32)),
        ("y0", pltpu.VMEM((width, points), BF16)),
        ("y1", pltpu.VMEM((width, points), BF16)),
        ("x", pltpu.VMEM((own_rows, points), F32)),
        ("tree", pltpu.VMEM((groups, own_rows, piece), F32)),
        ("cols", pltpu.VMEM((groups, own_rows, piece), F32)),
        ("cols_get", pltpu.VMEM((groups - 1, own_rows, piece), F32)),
        ("plain", pltpu.VMEM((2, groups // 2, own_rows, points), F32)),
        ("plain_fold", pltpu.VMEM((groups // 2, own_rows, points), F32)),
        ("plain_chip", pltpu.VMEM((groups // 2, own_rows, points), F32)),
        ("plain_get", pltpu.VMEM((max(1, groups // 2 - 1), own_rows, points), F32)),
        ("term", pltpu.VMEM((2, groups // 2, own_rows, width), F32)),
        ("term_fold", pltpu.VMEM((groups // 2, own_rows, width), F32)),
        ("term_chip", pltpu.VMEM((groups // 2, own_rows, width), F32)),
        ("term_get", pltpu.VMEM((max(1, groups // 2 - 1), own_rows, width), F32)),
        ("term_pass", pltpu.VMEM((own_rows, width), F32)),
        ("term_come", pltpu.VMEM((own_rows, width), F32)),
        ("g0", pltpu.VMEM((points, piece), BF16)),
        ("g1", pltpu.VMEM((points, piece), BF16)),
        ("g2", pltpu.VMEM((points, piece), BF16)),
        ("perm", pltpu.VMEM((points, points), BF16)),
    ]
    count = 6 + 3 * (groups // 2) - 2 + 4 * (levels - 1)
    for name, blocks in [*direct.items(), *slow.items()]:
        height = len(blocks) * rank
        items += [
            ("part_" + name, pltpu.VMEM((height, rank), F32)),
            ("fold_" + name, pltpu.VMEM((height // 2, rank), F32)),
            ("full_" + name, pltpu.VMEM((height, rank), F32)),
        ]
        if name in direct:
            count += 3
            items += [
                ("chip_" + name, pltpu.VMEM((height // 2, rank), F32)),
                ("peer_" + name, pltpu.VMEM((chips, height // 2, rank), F32)),
            ]
        else:
            stages = len(stages_of(name)) + chips
            count += 2 + len(stages_of(name))
            items += [
                ("pass_" + name, pltpu.VMEM((stages, height // 2, rank), F32)),
                ("come_" + name, pltpu.VMEM((stages, height // 2, rank), F32)),
            ]
    for h in range(1, levels):
        height = len(blocks_of(levels, h)) * rank
        items.append((f"send{h}", pltpu.VMEM((height, rank), F32)))
        items.append((f"get{h}", pltpu.VMEM((height, rank), F32)))
        height = (levels - h) * own_rows
        items.append((f"tsend{h}", pltpu.VMEM((height, rank), F32)))
        items.append((f"tget{h}", pltpu.VMEM((height, rank), F32)))
    items.append(("sent", pltpu.SemaphoreType.DMA((POOL + 3 * (groups // 2) - 1,))))
    items.append(("received", pltpu.SemaphoreType.DMA((count,))))
    return items


def scratch_names(cfg):
    return [name for name, _ in scratch_list(cfg)]


def local(right_sides, leaf_inverse, bases, ordering):
    own_rows, points = right_sides.shape
    levels, rank = bases.shape[:2]
    cfg = (
        lax.axis_size("leaf"),
        lax.axis_size("rhs"),
        levels,
        rank,
        own_rows,
        points,
        leaf_inverse.shape[1],
    )
    return pl.pallas_call(
        functools.partial(kernel, cfg),
        out_shape=pltpu.VMEM((own_rows, points), F32),
        in_specs=[pl.BlockSpec(memory_space=pl.ANY)] * 4,
        out_specs=pl.BlockSpec(memory_space=pltpu.VMEM),
        scratch_shapes=[item for _, item in scratch_list(cfg)],
        compiler_params=pltpu.CompilerParams(collective_id=0, has_side_effects=True),
        name="tree_solve",
    )(right_sides, leaf_inverse, bases, ordering)


def solution(mesh):
    placed = (P("rhs", "leaf"), P("leaf", "rhs"), P(None, None, "leaf"), P("leaf", None))
    return jax.shard_map(
        local, mesh=mesh, in_specs=placed, out_specs=P("rhs", "leaf"), check_vma=False
    )
```

```python
import functools
import itertools

import jax
import jax.numpy as jnp
from jax import lax
from jax.experimental import pallas as pl
from jax.experimental.pallas import tpu as pltpu
from jax.sharding import PartitionSpec as P

F32 = jnp.float32
BF16 = jnp.bfloat16
NN = (((1,), (0,)), ((), ()))
NT = (((1,), (1,)), ((), ()))
PANEL = 16
CHUNKS = 4
POOL = 12
ROWS, LANES = 8, 128
RADIX = 32


def split(value, pieces):
    parts = []
    for _ in range(pieces):
        head = value.astype(BF16)
        parts.append(head)
        value = value - head.astype(F32)
    return parts


def dot(left, right, dims):
    return lax.dot_general(left, right, dims, preferred_element_type=F32)


def fine(left, right, dims):
    return lax.dot_general(
        left, right, dims, precision=lax.Precision.HIGHEST, preferred_element_type=F32
    )


def inverse(matrix, hooks):
    size = matrix.shape[0]
    count = size // PANEL
    lane = lax.broadcasted_iota(jnp.int32, (PANEL, size), 1)
    row = lax.broadcasted_iota(jnp.int32, (PANEL, size), 0)
    zero = jnp.zeros((PANEL, size), F32)
    panels = [matrix[i * PANEL : (i + 1) * PANEL] for i in range(count)]

    def spread(panel, column):
        return jnp.broadcast_to(panel[:, column : column + 1], (PANEL, size))

    for i in range(count):
        for hook in hooks.get(i, ()):
            hook()
        start = i * PANEL
        inside = (lane >= start) & (lane < start + PANEL)
        panel = panels[i]
        columns = [spread(panel, start + k) for k in range(PANEL)]
        ahead = i + 1 < count
        if ahead:
            next_columns = [spread(panels[i + 1], start + k) for k in range(PANEL)]
        panel = jnp.where(inside, jnp.where(lane - start == row, 1.0, 0.0), panel)
        for k in range(PANEL):
            scale = 1.0 / columns[k][k : k + 1]
            at = row == k
            factor = jnp.where(at, -1.0, columns[k])
            panel = jnp.where(at, 0.0, panel) - factor * (panel[k : k + 1] * scale)
            for j in range(k + 1, PANEL):
                pivot = columns[j][k : k + 1] * scale
                columns[j] = jnp.where(at, 0.0, columns[j]) - factor * pivot
        padded = jnp.concatenate([zero] * i + [panel] + [zero] * (count - 1 - i), 0)
        update = fine(jnp.concatenate(panels, 0), padded, NN)
        if ahead:
            change = next_columns[0] * panel[0:1]
            for k in range(1, PANEL):
                change = change + next_columns[k] * panel[k : k + 1]
        for j in range(count):
            if j == i:
                panels[j] = panel
            else:
                own = update[j * PANEL : (j + 1) * PANEL]
                own = change if j == i + 1 else own
                panels[j] = jnp.where(inside, 0.0, panels[j]) - own
    return jnp.concatenate(panels, 0)


def blocks_of(levels, first):
    later = [(i, first) for i in range(first + 1, levels)]
    for j in range(first + 1, levels):
        later += [(i, j) for i in range(j, levels)]
    return [(first, first)] + later


def permute(value, index):
    tile = (ROWS, LANES)
    width = value.shape[1]
    bands = []
    for top in range(0, value.shape[0], ROWS):
        out = []
        for left in range(0, width, LANES):
            own = jnp.broadcast_to(index[:, left : left + LANES], tile)
            lane, block = lax.rem(own, LANES), lax.div(own, LANES)
            taken = None
            for source in range(width // LANES):
                part = value[top : top + ROWS, source * LANES : (source + 1) * LANES]
                part = jnp.take_along_axis(part, lane, axis=1)
                taken = part if taken is None else jnp.where(block == source, part, taken)
            out.append(taken)
        bands.append(jnp.concatenate(out, 1))
    return jnp.concatenate(bands, 0)


def layout(blocks, rank):
    spans, start = {}, 0
    for i, j in blocks:
        stop = start + (rank // 8 * 5 if i == j else rank)
        spans[i, j] = slice(start, stop)
        start = stop
    return spans, start


def pack(matrix):
    quarter = matrix.shape[0] // 4
    lane = lax.broadcasted_iota(jnp.int32, (1, 4 * quarter), 1)
    zero, one, two, three = (matrix[k * quarter : (k + 1) * quarter] for k in range(4))
    two = jnp.where(lane < 3 * quarter, two, pltpu.roll(zero, 3 * quarter, 1))
    low, high = one[: quarter // 2], one[quarter // 2 :]
    one = jnp.where(lane < 2 * quarter, low, pltpu.roll(high, 2 * quarter, 1))
    return jnp.concatenate([three, two, one], 0)


def unpack(packed):
    quarter = packed.shape[1] // 4
    three, two = packed[:quarter], packed[quarter : 2 * quarter]
    low = packed[2 * quarter :]
    lower = jnp.concatenate(
        [pltpu.roll(two, quarter, 1), low, pltpu.roll(low, 2 * quarter, 1), two, three], 0
    )
    upper = lower.T
    row = lax.broadcasted_iota(jnp.int32, (4 * quarter, 4 * quarter), 0)
    lane = lax.broadcasted_iota(jnp.int32, (4 * quarter, 4 * quarter), 1)
    return jnp.where(lane // quarter > row // quarter, upper, lower)


def direct_units(levels):
    units = {"c": [(0, 0)]}
    if levels > 1:
        units["a"] = [(1, 0), (1, 1)]
    if levels > 2:
        units["d"] = [(i, 0) for i in range(2, levels)]
    return units


def slow_units(levels):
    units = {}
    if levels > 2:
        units["e1"] = [(i, 1) for i in range(2, levels)]
    for j in range(2, levels):
        units[f"e{j}"] = [(i, j) for i in range(j, levels)]
    return units


def stages_of(name, groups):
    column = int(name[1:])
    stages = [(1 << h, 0) for h in range(1, column + 1)]
    stages += [(0, 1 << k) for k in range(1, groups.bit_length() - 1)]
    return stages + [(1, 0)]


def other(index, bit):
    return index + bit - 2 * bit * ((index // max(bit, 1)) % 2)


def kernel(cfg, rs_hbm, g_hbm, b_hbm, ord_hbm, out_ref, *scratch):
    leaves, groups, levels, rank, own_rows, points, piece = cfg
    rows = groups * own_rows
    ref = dict(zip(scratch_names(cfg), scratch))
    leaf, position = lax.axis_index("leaf"), lax.axis_index("rhs")
    mesh_id = pl.DeviceIdType.MESH
    direct, slow = direct_units(levels), slow_units(levels)

    def at(leaf_index, rhs_index):
        return {"leaf": leaf_index, "rhs": rhs_index}

    rhs_peers = [lax.rem(position + k, groups) for k in range(1, groups)]
    mate = other(position, 1)
    half = lax.rem(position, 2)
    chips = [(leaf, lax.rem(position + k, groups)) for k in range(2, groups, 2)]
    across = [peer for _, peer in chips]
    chips += [(other(leaf, 1), lax.rem(position + k, groups)) for k in range(0, groups, 2)]
    greeted = [(leaf, p) for p in rhs_peers]
    greeted += chips[groups // 2 - 1 :]
    greeted += [(other(leaf, 1 << h), position) for h in range(1, levels)]

    rs_ref, g_ref, b_ref, ord_ref = (ref[name] for name in ("rs", "g", "b", "ord"))
    chunk = points // CHUNKS
    moves = [(b_hbm.at[0], b_ref.at[0])]
    for k in range(CHUNKS):
        span = pl.ds(k * chunk, chunk)
        moves.append((g_hbm.at[span], g_ref.at[span]))
    moves += [(ord_hbm, ord_ref), (rs_hbm, rs_ref)]
    if levels > 1:
        later = pl.ds(1, levels - 1)
        moves.append((b_hbm.at[later], b_ref.at[later]))
    loads = [
        pltpu.make_async_copy(src, dst, ref["sent"].at[POOL - 1 - k]) for k, (src, dst) in enumerate(moves)
    ]
    urgent = CHUNKS + 1
    for load in loads[:urgent]:
        load.start()
    barrier = pltpu.get_barrier_semaphore()
    for target in greeted:
        pl.semaphore_signal(barrier, inc=1, device_id=at(*target), device_id_type=mesh_id)

    pool = {}
    turn = itertools.count()
    slots = itertools.count()

    def start(src, dst, target, receive, place):
        if place in pool:
            pool[place].wait_send()
        copy = pltpu.make_async_remote_copy(
            src_ref=src,
            dst_ref=dst,
            send_sem=ref["sent"].at[place],
            recv_sem=ref["received"].at[receive],
            device_id=at(*target),
            device_id_type=mesh_id,
        )
        copy.start()
        pool[place] = copy
        return copy

    def send(src, dst, target):
        return start(src, dst, target, next(slots), next(turn) % POOL)

    class Group:
        def __init__(self, copies, landed):
            receive = next(slots)
            for src, dst, target in copies:
                start(src, dst, target, receive, next(turn) % POOL)
            self.wait = pltpu.make_async_copy(landed, landed, ref["received"].at[receive])

        def wait_recv(self):
            self.wait.wait()

    def halves(buffer, which):
        count = buffer.shape[0] // 2
        return buffer.at[pl.ds(pl.multiple_of(which * count, count), count)]

    flying = {}

    def fold(name):
        part = halves(ref["part_" + name], 1 - half)
        flying[name] = send(part, ref["fold_" + name], (leaf, mate))

    def folded(name):
        flying[name].wait_recv()
        return halves(ref["part_" + name], half)[...] + ref["fold_" + name][...]

    def join(name, total):
        own = halves(ref["full_" + name], half)
        own[...] = total
        flying[name] = send(own, own, (leaf, mate))

    def scatter(name):
        ref["chip_" + name][...] = folded(name)
        peers = ref["peer_" + name]
        copies = [(ref["chip_" + name], peers.at[k], target) for k, target in enumerate(chips)]
        flying[name] = Group(copies, peers)

    def gather(name):
        total = ref["chip_" + name][...]
        flying[name].wait_recv()
        for k in range(len(chips)):
            total = total + ref["peer_" + name][k]
        join(name, total)

    def joined(name):
        flying[name].wait_recv()

    def slow_step(name, stage):
        stages = stages_of(name, groups)
        if stage == 0:
            total = folded(name)
        else:
            total = ref["pass_" + name][stage - 1]
            flying[name].wait_recv()
            total = total + ref["come_" + name][stage - 1]
        if stage == len(stages):
            join(name, total)
            return
        ref["pass_" + name][stage] = total
        leaf_bit, rhs_bit = stages[stage]
        target = (other(leaf, leaf_bit), other(position, rhs_bit))
        flying[name] = send(ref["pass_" + name].at[stage], ref["come_" + name].at[stage], target)

    todo = {}
    for name in slow:
        count = len(stages_of(name, groups))
        todo[name] = [functools.partial(slow_step, name, k) for k in range(count + 1)]
        todo[name].append(functools.partial(joined, name))

    def step(name, count=1):
        for _ in range(count):
            if todo.get(name):
                todo[name].pop(0)()

    def finish(name):
        while todo.get(name):
            step(name)

    own_cols = pl.ds(pl.multiple_of(position * piece, piece), piece)
    own_y = ref["y"].at[position]

    def products(left, parts):
        return dot(left, parts[0], NN) + (dot(left, parts[1], NN) + dot(left, parts[2], NN))

    def gram_of(solved, first, width):
        own_y[first * rank : first * rank + solved.shape[0]] = solved
        right = b_ref[:width, :, own_cols].reshape(width * rank, piece)
        return sum(dot(part, right, NT) for part in reversed(split(solved, 3)))

    def solved_of(first, last):
        left = b_ref[first:last].reshape((last - first) * rank, points)
        return products(left, [ref[f"g{k}"][...] for k in range(3)])

    loads[0].wait()
    solved = None
    for c in range(CHUNKS):
        loads[1 + c].wait()
        if c == CHUNKS // 2:
            loads[-1].start()
        if c == CHUNKS - 1:
            for load in loads[urgent : urgent + 2]:
                load.start()
        span = slice(c * chunk, (c + 1) * chunk)
        parts = split(g_ref[span], 3)
        for k, part in enumerate(parts):
            ref[f"g{k}"][span] = part
        value = products(b_ref[0, :, span], parts)
        solved = value if c == 0 else solved + value
    ref["part_c"][...] = pack(gram_of(solved, 0, 1))
    pl.semaphore_wait(barrier, len(greeted))
    fold("c")

    def arrange():
        for load in loads[urgent : urgent + 2]:
            load.wait()
        tree = permute(rs_ref[...], ord_ref[...])
        for k in range(groups):
            ref["tree"][k] = tree[:, k * piece : (k + 1) * piece]

    def invert_order():
        order = ord_ref[...]

        def one_hot(i, carry):
            start = pl.multiple_of(i * rank, rank)
            index = lax.broadcasted_iota(jnp.int32, (rank, points), 0) + start
            ref["perm"][pl.ds(start, rank), :] = jnp.where(index == order, 1.0, 0.0).astype(BF16)
            return carry

        lax.fori_loop(0, points // rank, one_hot, 0)
        row = lax.broadcasted_iota(jnp.int32, (2 * ROWS, points), 0)
        lane = lax.broadcasted_iota(jnp.int32, (2 * ROWS, points), 1)
        digits = jnp.where(row == 0, lax.div(lane, RADIX), lax.rem(lane, RADIX))
        found = dot(digits.astype(F32).astype(BF16), ref["perm"][...], NT)
        ref["back"][...] = (found[:1] * RADIX + found[1:2]).astype(jnp.int32)

    def part_store(gram, start, name, blocks):
        for (i, j), span in layout(blocks, rank)[0].items():
            block = gram[(i - start) * rank : (i - start + 1) * rank, j * rank : (j + 1) * rank]
            ref["part_" + name][span] = pack(block) if i == j else block

    if levels > 1:
        loads[urgent + 2].wait()
        solved = solved_of(1, 2)
    scatter("c")
    if levels > 1:
        part_store(gram_of(solved, 1, 2), 1, "a", direct["a"])
        fold("a")
    arrange()
    ref["cols"][position] = ref["tree"][position]
    copies = [
        (ref["tree"].at[peer], ref["cols_get"].at[k], (leaf, peer))
        for k, peer in enumerate(rhs_peers)
    ]
    pieces = Group(copies, ref["cols_get"])
    if levels > 2:
        gram = gram_of(solved_of(2, levels), 2, levels)
        later = {name: blocks for name, blocks in direct.items() if name not in "ca"}
        later |= slow
        for name, blocks in later.items():
            part_store(gram, 2, name, blocks)
        scatter("a")
        for name in later:
            fold(name)
    elif levels > 1:
        scatter("a")

    terms = []

    def term_part():
        pieces.wait_recv()
        for k in range(groups - 1):
            source = lax.rem(position + groups - 1 - k, groups)
            ref["cols"][source] = ref["cols_get"][k]
        columns = ref["cols"][...].reshape(rows, piece)
        term = fine(columns, own_y[...], NT)
        for k in range(groups):
            ref["term"][k % 2, k // 2] = term[k * own_rows : (k + 1) * own_rows]
        terms.append(send(ref["term"].at[1 - half], ref["term_fold"], (leaf, mate)))

    def term_cross():
        terms[0].wait_recv()
        ref["term_chip"][...] = ref["term"][half] + ref["term_fold"][...]
        for k, peer in enumerate(across):
            source = ref["term_chip"].at[lax.div(peer, 2)]
            terms.append(send(source, ref["term_get"].at[k], (leaf, peer)))

    def term_sum():
        total = ref["term_chip"][lax.div(position, 2)]
        for k, copy in enumerate(terms[1:]):
            copy.wait_recv()
            total = total + ref["term_get"][k]
        ref["term_pass"][...] = total
        terms.append(send(ref["term_pass"], ref["term_come"], (other(leaf, 1), position)))

    def term_joined():
        terms[-1].wait_recv()

    plain = []

    def plain_part():
        stack = jnp.concatenate(split(ref["cols"][...].reshape(rows, piece), 3), 0)
        by_0 = dot(stack, ref["g0"][...], NT)
        by_1 = dot(stack[: 2 * rows], ref["g1"][...], NT)
        by_2 = dot(stack[:rows], ref["g2"][...], NT)
        value = by_0[:rows] + (
            (by_0[rows : 2 * rows] + by_1[:rows]) + (by_0[2 * rows :] + by_1[rows:] + by_2)
        )
        for k in range(groups):
            ref["plain"][k % 2, k // 2] = value[k * own_rows : (k + 1) * own_rows]
        plain.append(send(ref["plain"].at[1 - half], ref["plain_fold"], (leaf, mate)))

    def plain_cross():
        plain[0].wait_recv()
        ref["plain_chip"][...] = ref["plain"][half] + ref["plain_fold"][...]
        for k, peer in enumerate(across):
            source = ref["plain_chip"].at[lax.div(peer, 2)]
            plain.append(send(source, ref["plain_get"].at[k], (leaf, peer)))

    def plain_sum():
        total = ref["plain_chip"][lax.div(position, 2)]
        for k, copy in enumerate(plain[1:]):
            copy.wait_recv()
            total = total + ref["plain_get"][k]
        ref["x"][...] = total

    solved_copies, relays = [], []

    def solved_across(first, last, place):
        part = own_y.at[pl.ds(first, last - first)]
        for k, peer in enumerate(across):
            solved_copies.append(start(part, part, (leaf, peer), next(slots), place + k))

    def solved_send(part):
        early = rank // 2
        if part == 0:
            solved_across(0, early, POOL)
        else:
            solved_across(early, levels * rank, POOL + len(across))
            place = POOL + 2 * len(across)
            relays.append(start(own_y, own_y, (leaf, mate), next(slots), place))

    def solved_relay():
        for copy in solved_copies:
            copy.wait_recv()
        for k in range(len(across)):
            source = lax.rem(position + groups - 2 * (k + 1), groups)
            slot = ref["y"].at[source]
            place = POOL + 2 * len(across) + 1 + k
            relays.append(start(slot, slot, (leaf, mate), next(slots), place))

    def solved_done():
        for copy in relays:
            copy.wait_recv()
        for k in range(groups):
            for p, part in enumerate(split(ref["y"][k], 2)):
                ref[f"y{p}"][:, k * piece : (k + 1) * piece] = part

    eye = (
        lax.broadcasted_iota(jnp.int32, (rank, rank), 0)
        == lax.broadcasted_iota(jnp.int32, (rank, rank), 1)
    ).astype(F32)
    linear = {}
    for name, blocks in [*direct.items(), *slow.items()]:
        for block, span in layout(blocks, rank)[0].items():
            linear[block] = (name, span)
    places = [layout(blocks_of(levels, h), rank)[0] for h in range(levels)]

    def linear_value(block):
        name, span = linear[block]
        return ref["full_" + name][span]

    def carried(h, block):
        span = places[h][block]
        return ref[f"send{h}"][span] + ref[f"get{h}"][span]

    def block_value(h, block):
        if h == 0:
            return linear_value(block)
        value = carried(h, block)
        return value if block == (1, 1) else value + linear_value(block)

    def term_value(h, j):
        if h == 0:
            span = slice(j * rank, (j + 1) * rank)
            return ref["term_pass"][:, span] + ref["term_come"][:, span]
        start = (j - h) * own_rows
        span = slice(start, start + own_rows)
        return ref[f"tsend{h}"][span] + ref[f"tget{h}"][span]

    level_copies = {}

    def level_send(h, part, start, stop):
        span = pl.ds(start, stop - start)
        level_copies[h, part] = send(
            ref[f"send{h}"].at[span], ref[f"get{h}"].at[span], (other(leaf, 1 << h), position)
        )

    def level_wait(h, part):
        copy = level_copies.pop((h, part), None)
        if copy is not None:
            copy.wait_recv()

    inverses = [None] * levels
    below = [None] * levels
    weights = {}
    term_weights = {}

    def level_terms(h):
        if h:
            level_wait(h, "terms")
        own = term_value(h, h)
        term_weights[h] = fine(own, inverses[h], NN)
        if h + 1 < levels:
            for k, j in enumerate(range(h + 1, levels)):
                change = fine(own, weights[j, h], NT)
                span = slice(k * own_rows, (k + 1) * own_rows)
                ref[f"tsend{h + 1}"][span] = term_value(h, j) - change

    def terms_send(h):
        level_copies[h + 1, "terms"] = send(
            ref[f"tsend{h + 1}"], ref[f"tget{h + 1}"], (other(leaf, 2 << h), position)
        )

    def level_change(h, block):
        i, j = block
        change = fine(weights[i, h], below[h][j], NT)
        if i == j:
            change = pack(change)
        if block == (1, 1):
            return linear_value(block) - change
        return carried(h, block) - change if h else -change

    def level_span(h, first, last):
        return [(block, places[h][block]) for block in blocks_of(levels, h)[first:last]]

    def level_column(h):
        level_wait(h, "rest")
        spans = level_span(h + 1, 1, levels - h - 1)
        for (i, j), span in spans:
            change = fine(below[h][i], weights[j, h], NT)
            ref[f"send{h + 1}"][span] = carried(h, (i, j)) - change if h else -change
        level_send(h + 1, "column", spans[0][1].start, spans[-1][1].stop)

    def level_rest(h):
        for i in range(h + 2, levels):
            weights[i, h] = fine(below[h][i], inverses[h], NN)
        for block, span in level_span(h + 1, levels - h - 1, None):
            ref[f"send{h + 1}"][span] = level_change(h, block)

    def level_rest_send(h):
        spans = level_span(h + 1, levels - h - 1, None)
        level_send(h + 1, "rest", spans[0][1].start, spans[-1][1].stop)


    for name in slow:
        step(name)
    gather("c")
    term_part()
    joined("c")
    hooks = {h: {} for h in range(levels)}
    if levels > 1:
        hooks[0] = {5: [lambda: gather("a")]}
    if levels > 2:
        hooks[0][1] = [lambda: scatter("d")]
        hooks[0][3] = [term_cross]
        hooks[0][4] = [lambda: step("e1"), lambda: step("e2")]
        hooks[1] = {
            3: [lambda: step("e1")],
            6: [lambda: step("e2"), term_joined, lambda: level_terms(0)],
            7: [lambda: terms_send(0)],
        }
    else:
        hooks[0][2] = [term_cross]
    carry, partial = [None] * levels, [None] * levels
    for h in range(levels):
        last = h == levels - 1
        if h:
            level_wait(h, "head")
            if h > 1:
                finish(f"e{h}")
        if last:
            if h == 0:
                term_sum()
                solved_send(0)
                solved_send(1)
                plain_part()
                plain_cross()
                term_joined()
                solved_relay()
                invert_order()
            hooks[h][7] = [solved_done]
        inverses[h] = inverse(unpack(block_value(h, (h, h))) + eye, hooks[h])
        if last:
            break
        if h == 0:
            joined("a")
        else:
            level_wait(h, "column")
            finish(f"e{h}")
        first = block_value(h, (h + 1, h))
        below[h] = {h + 1: first}
        weights[h + 1, h] = fine(first, inverses[h], NN)
        if h:
            level_wait(h, "rest")
        span = places[h + 1][h + 1, h + 1]
        ref[f"send{h + 1}"][span] = level_change(h, (h + 1, h + 1))
        level_send(h + 1, "head", span.start, span.stop)
        if h + 2 < levels:
            if h == 0:
                solved_send(0)
                gather("d")
                step("e1")
                plain_part()
                step("e2")
                solved_send(1)
                joined("d")
            for i in range(h + 2, levels):
                below[h][i] = block_value(h, (i, h))
            level_column(h)
            if h == 0:
                hooks[1][1] = [lambda: level_rest(0)]
                hooks[1][2] = [lambda: level_rest_send(0)]
            else:
                level_rest(h)
                level_rest_send(h)
        if h == 0:
            term_sum()
            if levels == 2:
                solved_send(0)
                solved_send(1)
                plain_part()
        if h or levels == 2:
            if h == 0:
                term_joined()
            if h == levels - 2:
                step("e2")
                plain_cross()
                invert_order()
            level_terms(h)
            terms_send(h)
        if h == levels - 2:
            for k in reversed(range(levels - 1)):
                carry[k] = weights[levels - 1, k]
                partial[k] = term_weights[k]
                for j in range(k + 1, levels - 1):
                    carry[k] = carry[k] - fine(carry[j], weights[j, k], NN)
                    partial[k] = partial[k] - fine(partial[j], weights[j, k], NN)
            solved_relay()
    level_terms(levels - 1)
    plain_sum()

    coefficients = [term_weights[levels - 1] if h == levels - 1 else partial[h] for h in range(levels)]
    for h in range(levels - 1):
        coefficients[h] = coefficients[h] - fine(coefficients[levels - 1], carry[h], NN)
    stack = jnp.concatenate(split(jnp.concatenate(coefficients, 1), 2), 0)
    by_0 = dot(stack, ref["y0"][...], NN)
    by_1 = dot(stack[:own_rows], ref["y1"][...], NN)
    tree_rows = ref["x"][...] - (by_0[:own_rows] + (by_0[own_rows:] + by_1))
    out_ref[...] = permute(tree_rows, ref["back"][...])

    for copy in pool.values():
        copy.wait_send()


def scratch_list(cfg):
    leaves, groups, levels, rank, own_rows, points, piece = cfg
    chips = groups - 1
    width = levels * rank
    direct, slow = direct_units(levels), slow_units(levels)
    items = [
        ("rs", pltpu.VMEM((own_rows, points), F32)),
        ("g", pltpu.VMEM((points, piece), F32)),
        ("b", pltpu.VMEM((levels, rank, points), BF16)),
        ("ord", pltpu.VMEM((1, points), jnp.int32)),
        ("y", pltpu.VMEM((groups, width, piece), F32)),
        ("y0", pltpu.VMEM((width, points), BF16)),
        ("y1", pltpu.VMEM((width, points), BF16)),
        ("x", pltpu.VMEM((own_rows, points), F32)),
        ("tree", pltpu.VMEM((groups, own_rows, piece), F32)),
        ("cols", pltpu.VMEM((groups, own_rows, piece), F32)),
        ("cols_get", pltpu.VMEM((groups - 1, own_rows, piece), F32)),
        ("plain", pltpu.VMEM((2, groups // 2, own_rows, points), F32)),
        ("plain_fold", pltpu.VMEM((groups // 2, own_rows, points), F32)),
        ("plain_chip", pltpu.VMEM((groups // 2, own_rows, points), F32)),
        ("plain_get", pltpu.VMEM((max(1, groups // 2 - 1), own_rows, points), F32)),
        ("term", pltpu.VMEM((2, groups // 2, own_rows, width), F32)),
        ("term_fold", pltpu.VMEM((groups // 2, own_rows, width), F32)),
        ("term_chip", pltpu.VMEM((groups // 2, own_rows, width), F32)),
        ("term_get", pltpu.VMEM((max(1, groups // 2 - 1), own_rows, width), F32)),
        ("term_pass", pltpu.VMEM((own_rows, width), F32)),
        ("term_come", pltpu.VMEM((own_rows, width), F32)),
        ("g0", pltpu.VMEM((points, piece), BF16)),
        ("g1", pltpu.VMEM((points, piece), BF16)),
        ("g2", pltpu.VMEM((points, piece), BF16)),
        ("perm", pltpu.VMEM((points, points), BF16)),
        ("back", pltpu.VMEM((1, points), jnp.int32)),
    ]
    count = 6 + 3 * (groups // 2) - 2 + 4 * (levels - 1)
    for name, blocks in [*direct.items(), *slow.items()]:
        height = layout(blocks, rank)[1]
        items += [
            ("part_" + name, pltpu.VMEM((height, rank), F32)),
            ("fold_" + name, pltpu.VMEM((height // 2, rank), F32)),
            ("full_" + name, pltpu.VMEM((height, rank), F32)),
        ]
        if name in direct:
            count += 3
            items += [
                ("chip_" + name, pltpu.VMEM((height // 2, rank), F32)),
                ("peer_" + name, pltpu.VMEM((chips, height // 2, rank), F32)),
            ]
        else:
            stages = len(stages_of(name, groups))
            count += 2 + stages
            items += [
                ("pass_" + name, pltpu.VMEM((stages, height // 2, rank), F32)),
                ("come_" + name, pltpu.VMEM((stages, height // 2, rank), F32)),
            ]
    for h in range(1, levels):
        height = layout(blocks_of(levels, h), rank)[1]
        items.append((f"send{h}", pltpu.VMEM((height, rank), F32)))
        items.append((f"get{h}", pltpu.VMEM((height, rank), F32)))
        height = (levels - h) * own_rows
        items.append((f"tsend{h}", pltpu.VMEM((height, rank), F32)))
        items.append((f"tget{h}", pltpu.VMEM((height, rank), F32)))
    items.append(("sent", pltpu.SemaphoreType.DMA((POOL + 3 * (groups // 2) - 1,))))
    items.append(("received", pltpu.SemaphoreType.DMA((count,))))
    return items


def scratch_names(cfg):
    return [name for name, _ in scratch_list(cfg)]


def local(right_sides, leaf_inverse, bases, ordering):
    own_rows, points = right_sides.shape
    levels, rank = bases.shape[:2]
    cfg = (
        lax.axis_size("leaf"),
        lax.axis_size("rhs"),
        levels,
        rank,
        own_rows,
        points,
        leaf_inverse.shape[1],
    )
    return pl.pallas_call(
        functools.partial(kernel, cfg),
        out_shape=pltpu.VMEM((own_rows, points), F32),
        in_specs=[pl.BlockSpec(memory_space=pl.ANY)] * 4,
        out_specs=pl.BlockSpec(memory_space=pltpu.VMEM),
        scratch_shapes=[item for _, item in scratch_list(cfg)],
        compiler_params=pltpu.CompilerParams(collective_id=0, has_side_effects=True),
        name="tree_solve",
    )(right_sides, leaf_inverse, bases, ordering)


def solution(mesh):
    placed = (P("rhs", "leaf"), P("leaf", "rhs"), P(None, None, "leaf"), P("leaf", None))
    return jax.shard_map(
        local, mesh=mesh, in_specs=placed, out_specs=P("rhs", "leaf"), check_vma=False
    )
```

```python
import functools
import itertools

import jax
import jax.numpy as jnp
from jax import lax
from jax.experimental import pallas as pl
from jax.experimental.pallas import tpu as pltpu
from jax.sharding import PartitionSpec as P

F32 = jnp.float32
BF16 = jnp.bfloat16
NN = (((1,), (0,)), ((), ()))
NT = (((1,), (1,)), ((), ()))
PANEL = 16
CHUNKS = 4
POOL = 12
ROWS, LANES = 8, 128
RADIX = 32


def split(value, pieces):
    parts = []
    for _ in range(pieces):
        head = value.astype(BF16)
        parts.append(head)
        value = value - head.astype(F32)
    return parts


def dot(left, right, dims):
    return lax.dot_general(left, right, dims, preferred_element_type=F32)


def fine(left, right, dims):
    return lax.dot_general(
        left, right, dims, precision=lax.Precision.HIGHEST, preferred_element_type=F32
    )


def coarse(left, right, dims):
    first, second = split(left, 2)
    upper, lower = split(right, 2)
    return dot(first, upper, dims) + (dot(second, upper, dims) + dot(first, lower, dims))


def inverse(matrix, hooks):
    size = matrix.shape[0]
    count = size // PANEL
    lane = lax.broadcasted_iota(jnp.int32, (PANEL, size), 1)
    row = lax.broadcasted_iota(jnp.int32, (PANEL, size), 0)
    zero = jnp.zeros((PANEL, size), F32)
    panels = [matrix[i * PANEL : (i + 1) * PANEL] for i in range(count)]

    def spread(panel, column):
        return jnp.broadcast_to(panel[:, column : column + 1], (PANEL, size))

    for i in range(count):
        for hook in hooks.get(i, ()):
            hook()
        start = i * PANEL
        inside = (lane >= start) & (lane < start + PANEL)
        panel = panels[i]
        columns = [spread(panel, start + k) for k in range(PANEL)]
        ahead = i + 1 < count
        if ahead:
            next_columns = [spread(panels[i + 1], start + k) for k in range(PANEL)]
        panel = jnp.where(inside, jnp.where(lane - start == row, 1.0, 0.0), panel)
        for k in range(PANEL):
            scale = 1.0 / columns[k][k : k + 1]
            at = row == k
            factor = jnp.where(at, -1.0, columns[k])
            panel = jnp.where(at, 0.0, panel) - factor * (panel[k : k + 1] * scale)
            for j in range(k + 1, PANEL):
                pivot = columns[j][k : k + 1] * scale
                columns[j] = jnp.where(at, 0.0, columns[j]) - factor * pivot
        padded = jnp.concatenate([zero] * i + [panel] + [zero] * (count - 1 - i), 0)
        update = coarse(jnp.concatenate(panels, 0), padded, NN)
        if ahead:
            change = next_columns[0] * panel[0:1]
            for k in range(1, PANEL):
                change = change + next_columns[k] * panel[k : k + 1]
        for j in range(count):
            if j == i:
                panels[j] = panel
            else:
                own = update[j * PANEL : (j + 1) * PANEL]
                own = change if j == i + 1 else own
                panels[j] = jnp.where(inside, 0.0, panels[j]) - own
    return jnp.concatenate(panels, 0)


def blocks_of(levels, first):
    later = [(i, first) for i in range(first + 1, levels)]
    for j in range(first + 1, levels):
        later += [(i, j) for i in range(j, levels)]
    return [(first, first)] + later


def permute(value, index):
    tile = (ROWS, LANES)
    width = value.shape[1]
    bands = []
    for top in range(0, value.shape[0], ROWS):
        out = []
        for left in range(0, width, LANES):
            own = jnp.broadcast_to(index[:, left : left + LANES], tile)
            lane, block = lax.rem(own, LANES), lax.div(own, LANES)
            taken = None
            for source in range(width // LANES):
                part = value[top : top + ROWS, source * LANES : (source + 1) * LANES]
                part = jnp.take_along_axis(part, lane, axis=1)
                taken = part if taken is None else jnp.where(block == source, part, taken)
            out.append(taken)
        bands.append(jnp.concatenate(out, 1))
    return jnp.concatenate(bands, 0)


def layout(blocks, rank):
    spans, start = {}, 0
    for i, j in blocks:
        stop = start + (rank // 8 * 5 if i == j else rank)
        spans[i, j] = slice(start, stop)
        start = stop
    return spans, start


def pack(matrix):
    quarter = matrix.shape[0] // 4
    lane = lax.broadcasted_iota(jnp.int32, (1, 4 * quarter), 1)
    zero, one, two, three = (matrix[k * quarter : (k + 1) * quarter] for k in range(4))
    two = jnp.where(lane < 3 * quarter, two, pltpu.roll(zero, 3 * quarter, 1))
    low, high = one[: quarter // 2], one[quarter // 2 :]
    one = jnp.where(lane < 2 * quarter, low, pltpu.roll(high, 2 * quarter, 1))
    return jnp.concatenate([three, two, one], 0)


def unpack(packed):
    quarter = packed.shape[1] // 4
    three, two = packed[:quarter], packed[quarter : 2 * quarter]
    low = packed[2 * quarter :]
    lower = jnp.concatenate(
        [pltpu.roll(two, quarter, 1), low, pltpu.roll(low, 2 * quarter, 1), two, three], 0
    )
    upper = lower.T
    row = lax.broadcasted_iota(jnp.int32, (4 * quarter, 4 * quarter), 0)
    lane = lax.broadcasted_iota(jnp.int32, (4 * quarter, 4 * quarter), 1)
    return jnp.where(lane // quarter > row // quarter, upper, lower)


def direct_units(levels):
    units = {"c": [(0, 0)]}
    if levels > 1:
        units["a"] = [(1, 0), (1, 1)]
    if levels > 2:
        units["d"] = [(i, 0) for i in range(2, levels)]
    return units


def slow_units(levels):
    units = {}
    if levels > 2:
        units["e1"] = [(i, 1) for i in range(2, levels)]
    for j in range(2, levels):
        units[f"e{j}"] = [(i, j) for i in range(j, levels)]
    return units


def stages_of(name, groups):
    column = int(name[1:])
    stages = [(1 << h, 0) for h in range(1, column + 1)]
    stages += [(0, 1 << k) for k in range(1, groups.bit_length() - 1)]
    return stages + [(1, 0)]


def other(index, bit):
    return index + bit - 2 * bit * ((index // max(bit, 1)) % 2)


def kernel(cfg, rs_hbm, g_hbm, b_hbm, ord_hbm, out_ref, *scratch):
    leaves, groups, levels, rank, own_rows, points, piece = cfg
    rows = groups * own_rows
    ref = dict(zip(scratch_names(cfg), scratch))
    leaf, position = lax.axis_index("leaf"), lax.axis_index("rhs")
    mesh_id = pl.DeviceIdType.MESH
    direct, slow = direct_units(levels), slow_units(levels)

    def at(leaf_index, rhs_index):
        return {"leaf": leaf_index, "rhs": rhs_index}

    rhs_peers = [lax.rem(position + k, groups) for k in range(1, groups)]
    mate = other(position, 1)
    half = lax.rem(position, 2)
    chips = [(leaf, lax.rem(position + k, groups)) for k in range(2, groups, 2)]
    across = [peer for _, peer in chips]
    chips += [(other(leaf, 1), lax.rem(position + k, groups)) for k in range(0, groups, 2)]
    greeted = [(leaf, p) for p in rhs_peers]
    greeted += chips[groups // 2 - 1 :]
    greeted += [(other(leaf, 1 << h), position) for h in range(1, levels)]

    rs_ref, g_ref, b_ref, ord_ref = (ref[name] for name in ("rs", "g", "b", "ord"))
    chunk = points // CHUNKS
    moves = [(b_hbm.at[0], b_ref.at[0])]
    for k in range(CHUNKS):
        span = pl.ds(k * chunk, chunk)
        moves.append((g_hbm.at[span], g_ref.at[span]))
    moves += [(ord_hbm, ord_ref), (rs_hbm, rs_ref)]
    if levels > 1:
        later = pl.ds(1, levels - 1)
        moves.append((b_hbm.at[later], b_ref.at[later]))
    loads = [
        pltpu.make_async_copy(src, dst, ref["sent"].at[POOL - 1 - k]) for k, (src, dst) in enumerate(moves)
    ]
    urgent = CHUNKS + 1
    for load in loads[:urgent]:
        load.start()
    barrier = pltpu.get_barrier_semaphore()
    for target in greeted:
        pl.semaphore_signal(barrier, inc=1, device_id=at(*target), device_id_type=mesh_id)

    pool = {}
    turn = itertools.count()
    slots = itertools.count()

    def start(src, dst, target, receive, place):
        if place in pool:
            pool[place].wait_send()
        copy = pltpu.make_async_remote_copy(
            src_ref=src,
            dst_ref=dst,
            send_sem=ref["sent"].at[place],
            recv_sem=ref["received"].at[receive],
            device_id=at(*target),
            device_id_type=mesh_id,
        )
        copy.start()
        pool[place] = copy
        return copy

    def send(src, dst, target):
        return start(src, dst, target, next(slots), next(turn) % POOL)

    class Group:
        def __init__(self, copies, landed):
            receive = next(slots)
            for src, dst, target in copies:
                start(src, dst, target, receive, next(turn) % POOL)
            self.wait = pltpu.make_async_copy(landed, landed, ref["received"].at[receive])

        def wait_recv(self):
            self.wait.wait()

    def halves(buffer, which):
        count = buffer.shape[0] // 2
        return buffer.at[pl.ds(pl.multiple_of(which * count, count), count)]

    flying = {}

    def fold(name):
        part = halves(ref["part_" + name], 1 - half)
        flying[name] = send(part, ref["fold_" + name], (leaf, mate))

    def folded(name):
        flying[name].wait_recv()
        return halves(ref["part_" + name], half)[...] + ref["fold_" + name][...]

    def join(name, total):
        own = halves(ref["full_" + name], half)
        own[...] = total
        flying[name] = send(own, own, (leaf, mate))

    def scatter(name):
        ref["chip_" + name][...] = folded(name)
        peers = ref["peer_" + name]
        copies = [(ref["chip_" + name], peers.at[k], target) for k, target in enumerate(chips)]
        flying[name] = Group(copies, peers)

    def gather(name):
        total = ref["chip_" + name][...]
        flying[name].wait_recv()
        for k in range(len(chips)):
            total = total + ref["peer_" + name][k]
        join(name, total)

    def joined(name):
        flying[name].wait_recv()

    def slow_step(name, stage):
        stages = stages_of(name, groups)
        if stage == 0:
            total = folded(name)
        else:
            total = ref["pass_" + name][stage - 1]
            flying[name].wait_recv()
            total = total + ref["come_" + name][stage - 1]
        if stage == len(stages):
            join(name, total)
            return
        ref["pass_" + name][stage] = total
        leaf_bit, rhs_bit = stages[stage]
        target = (other(leaf, leaf_bit), other(position, rhs_bit))
        flying[name] = send(ref["pass_" + name].at[stage], ref["come_" + name].at[stage], target)

    todo = {}
    for name in slow:
        count = len(stages_of(name, groups))
        todo[name] = [functools.partial(slow_step, name, k) for k in range(count + 1)]
        todo[name].append(functools.partial(joined, name))

    def step(name, count=1):
        for _ in range(count):
            if todo.get(name):
                todo[name].pop(0)()

    def finish(name):
        while todo.get(name):
            step(name)

    own_cols = pl.ds(pl.multiple_of(position * piece, piece), piece)
    own_y = ref["y"].at[position]

    def products(left, parts):
        return dot(left, parts[0], NN) + (dot(left, parts[1], NN) + dot(left, parts[2], NN))

    def gram_of(solved, first, width):
        own_y[first * rank : first * rank + solved.shape[0]] = solved
        right = b_ref[:width, :, own_cols].reshape(width * rank, piece)
        return sum(dot(part, right, NT) for part in reversed(split(solved, 3)))

    def solved_of(first, last):
        left = b_ref[first:last].reshape((last - first) * rank, points)
        return products(left, [ref[f"g{k}"][...] for k in range(3)])

    loads[0].wait()
    solved = None
    for c in range(CHUNKS):
        loads[1 + c].wait()
        if c == CHUNKS // 2:
            loads[-1].start()
        if c == CHUNKS - 1:
            for load in loads[urgent : urgent + 2]:
                load.start()
        span = slice(c * chunk, (c + 1) * chunk)
        parts = split(g_ref[span], 3)
        for k, part in enumerate(parts):
            ref[f"g{k}"][span] = part
        value = products(b_ref[0, :, span], parts)
        solved = value if c == 0 else solved + value
    ref["part_c"][...] = pack(gram_of(solved, 0, 1))
    pl.semaphore_wait(barrier, len(greeted))
    fold("c")

    def arrange():
        for load in loads[urgent : urgent + 2]:
            load.wait()
        tree = permute(rs_ref[...], ord_ref[...])
        for k in range(groups):
            ref["tree"][k] = tree[:, k * piece : (k + 1) * piece]

    def invert_order():
        order = ord_ref[...]

        def one_hot(i, carry):
            start = pl.multiple_of(i * rank, rank)
            index = lax.broadcasted_iota(jnp.int32, (rank, points), 0) + start
            ref["perm"][pl.ds(start, rank), :] = jnp.where(index == order, 1.0, 0.0).astype(BF16)
            return carry

        lax.fori_loop(0, points // rank, one_hot, 0)
        row = lax.broadcasted_iota(jnp.int32, (2 * ROWS, points), 0)
        lane = lax.broadcasted_iota(jnp.int32, (2 * ROWS, points), 1)
        digits = jnp.where(row == 0, lax.div(lane, RADIX), lax.rem(lane, RADIX))
        found = dot(digits.astype(F32).astype(BF16), ref["perm"][...], NT)
        ref["back"][...] = (found[:1] * RADIX + found[1:2]).astype(jnp.int32)

    def part_store(gram, start, name, blocks):
        for (i, j), span in layout(blocks, rank)[0].items():
            block = gram[(i - start) * rank : (i - start + 1) * rank, j * rank : (j + 1) * rank]
            ref["part_" + name][span] = pack(block) if i == j else block

    if levels > 1:
        loads[urgent + 2].wait()
        solved = solved_of(1, 2)
    scatter("c")
    if levels > 1:
        part_store(gram_of(solved, 1, 2), 1, "a", direct["a"])
        fold("a")
    arrange()
    ref["cols"][position] = ref["tree"][position]
    copies = [
        (ref["tree"].at[peer], ref["cols_get"].at[k], (leaf, peer))
        for k, peer in enumerate(rhs_peers)
    ]
    pieces = Group(copies, ref["cols_get"])
    if levels > 2:
        gram = gram_of(solved_of(2, levels), 2, levels)
        later = {name: blocks for name, blocks in direct.items() if name not in "ca"}
        later |= slow
        for name, blocks in later.items():
            part_store(gram, 2, name, blocks)
        scatter("a")
        for name in later:
            fold(name)
    elif levels > 1:
        scatter("a")

    terms = []

    def term_part():
        pieces.wait_recv()
        for k in range(groups - 1):
            source = lax.rem(position + groups - 1 - k, groups)
            ref["cols"][source] = ref["cols_get"][k]
        columns = ref["cols"][...].reshape(rows, piece)
        term = fine(columns, own_y[...], NT)
        for k in range(groups):
            ref["term"][k % 2, k // 2] = term[k * own_rows : (k + 1) * own_rows]
        terms.append(send(ref["term"].at[1 - half], ref["term_fold"], (leaf, mate)))

    def term_cross():
        terms[0].wait_recv()
        ref["term_chip"][...] = ref["term"][half] + ref["term_fold"][...]
        for k, peer in enumerate(across):
            source = ref["term_chip"].at[lax.div(peer, 2)]
            terms.append(send(source, ref["term_get"].at[k], (leaf, peer)))

    def term_sum():
        total = ref["term_chip"][lax.div(position, 2)]
        for k, copy in enumerate(terms[1:]):
            copy.wait_recv()
            total = total + ref["term_get"][k]
        ref["term_pass"][...] = total
        terms.append(send(ref["term_pass"], ref["term_come"], (other(leaf, 1), position)))

    def term_joined():
        terms[-1].wait_recv()

    plain = []

    def plain_part():
        stack = jnp.concatenate(split(ref["cols"][...].reshape(rows, piece), 3), 0)
        by_0 = dot(stack, ref["g0"][...], NT)
        by_1 = dot(stack[: 2 * rows], ref["g1"][...], NT)
        by_2 = dot(stack[:rows], ref["g2"][...], NT)
        value = by_0[:rows] + (
            (by_0[rows : 2 * rows] + by_1[:rows]) + (by_0[2 * rows :] + by_1[rows:] + by_2)
        )
        for k in range(groups):
            ref["plain"][k % 2, k // 2] = value[k * own_rows : (k + 1) * own_rows]
        plain.append(send(ref["plain"].at[1 - half], ref["plain_fold"], (leaf, mate)))

    def plain_cross():
        plain[0].wait_recv()
        ref["plain_chip"][...] = ref["plain"][half] + ref["plain_fold"][...]
        for k, peer in enumerate(across):
            source = ref["plain_chip"].at[lax.div(peer, 2)]
            plain.append(send(source, ref["plain_get"].at[k], (leaf, peer)))

    def plain_sum():
        total = ref["plain_chip"][lax.div(position, 2)]
        for k, copy in enumerate(plain[1:]):
            copy.wait_recv()
            total = total + ref["plain_get"][k]
        ref["x"][...] = total

    solved_copies, relays = [], []

    def solved_across(first, last, place):
        part = own_y.at[pl.ds(first, last - first)]
        for k, peer in enumerate(across):
            solved_copies.append(start(part, part, (leaf, peer), next(slots), place + k))

    def solved_send(part):
        early = rank // 2
        if part == 0:
            solved_across(0, early, POOL)
        else:
            solved_across(early, levels * rank, POOL + len(across))
            place = POOL + 2 * len(across)
            relays.append(start(own_y, own_y, (leaf, mate), next(slots), place))

    def solved_relay():
        for copy in solved_copies:
            copy.wait_recv()
        for k in range(len(across)):
            source = lax.rem(position + groups - 2 * (k + 1), groups)
            slot = ref["y"].at[source]
            place = POOL + 2 * len(across) + 1 + k
            relays.append(start(slot, slot, (leaf, mate), next(slots), place))

    def solved_done():
        for copy in relays:
            copy.wait_recv()
        for k in range(groups):
            for p, part in enumerate(split(ref["y"][k], 2)):
                ref[f"y{p}"][:, k * piece : (k + 1) * piece] = part

    eye = (
        lax.broadcasted_iota(jnp.int32, (rank, rank), 0)
        == lax.broadcasted_iota(jnp.int32, (rank, rank), 1)
    ).astype(F32)
    linear = {}
    for name, blocks in [*direct.items(), *slow.items()]:
        for block, span in layout(blocks, rank)[0].items():
            linear[block] = (name, span)
    places = [layout(blocks_of(levels, h), rank)[0] for h in range(levels)]

    def linear_value(block):
        name, span = linear[block]
        return ref["full_" + name][span]

    def carried(h, block):
        span = places[h][block]
        return ref[f"send{h}"][span] + ref[f"get{h}"][span]

    def block_value(h, block):
        if h == 0:
            return linear_value(block)
        value = carried(h, block)
        return value if block == (1, 1) else value + linear_value(block)

    def term_value(h, j):
        if h == 0:
            span = slice(j * rank, (j + 1) * rank)
            return ref["term_pass"][:, span] + ref["term_come"][:, span]
        start = (j - h) * own_rows
        span = slice(start, start + own_rows)
        return ref[f"tsend{h}"][span] + ref[f"tget{h}"][span]

    level_copies = {}

    def level_send(h, part, start, stop):
        span = pl.ds(start, stop - start)
        level_copies[h, part] = send(
            ref[f"send{h}"].at[span], ref[f"get{h}"].at[span], (other(leaf, 1 << h), position)
        )

    def level_wait(h, part):
        copy = level_copies.pop((h, part), None)
        if copy is not None:
            copy.wait_recv()

    inverses = [None] * levels
    below = [None] * levels
    weights = {}
    term_weights = {}

    def level_terms(h):
        if h:
            level_wait(h, "terms")
        own = term_value(h, h)
        term_weights[h] = coarse(own, inverses[h], NN)
        if h + 1 < levels:
            for k, j in enumerate(range(h + 1, levels)):
                change = coarse(own, weights[j, h], NT)
                span = slice(k * own_rows, (k + 1) * own_rows)
                ref[f"tsend{h + 1}"][span] = term_value(h, j) - change

    def terms_send(h):
        level_copies[h + 1, "terms"] = send(
            ref[f"tsend{h + 1}"], ref[f"tget{h + 1}"], (other(leaf, 2 << h), position)
        )

    def level_change(h, block):
        i, j = block
        change = coarse(weights[i, h], below[h][j], NT)
        if i == j:
            change = pack(change)
        if block == (1, 1):
            return linear_value(block) - change
        return carried(h, block) - change if h else -change

    def level_span(h, first, last):
        return [(block, places[h][block]) for block in blocks_of(levels, h)[first:last]]

    def level_column(h):
        level_wait(h, "rest")
        spans = level_span(h + 1, 1, levels - h - 1)
        for (i, j), span in spans:
            change = coarse(below[h][i], weights[j, h], NT)
            ref[f"send{h + 1}"][span] = carried(h, (i, j)) - change if h else -change
        level_send(h + 1, "column", spans[0][1].start, spans[-1][1].stop)

    def level_rest(h):
        for i in range(h + 2, levels):
            weights[i, h] = coarse(below[h][i], inverses[h], NN)
        for block, span in level_span(h + 1, levels - h - 1, None):
            ref[f"send{h + 1}"][span] = level_change(h, block)

    def level_rest_send(h):
        spans = level_span(h + 1, levels - h - 1, None)
        level_send(h + 1, "rest", spans[0][1].start, spans[-1][1].stop)


    for name in slow:
        step(name)
    gather("c")
    term_part()
    joined("c")
    hooks = {h: {} for h in range(levels)}
    if levels > 1:
        hooks[0] = {5: [lambda: gather("a")]}
    if levels > 2:
        hooks[0][1] = [lambda: scatter("d")]
        hooks[0][3] = [term_cross]
        hooks[0][4] = [lambda: step("e1"), lambda: step("e2")]
        hooks[1] = {
            3: [lambda: step("e1")],
            5: [lambda: step("e2"), term_joined, lambda: level_terms(0)],
            6: [lambda: terms_send(0)],
        }
    else:
        hooks[0][2] = [term_cross]
    carry, partial = [None] * levels, [None] * levels
    for h in range(levels):
        last = h == levels - 1
        if h:
            level_wait(h, "head")
            if h > 1:
                finish(f"e{h}")
        if last:
            if h == 0:
                term_sum()
                solved_send(0)
                solved_send(1)
                plain_part()
                plain_cross()
                term_joined()
                solved_relay()
                invert_order()
            hooks[h][7] = [solved_done]
        inverses[h] = inverse(unpack(block_value(h, (h, h))) + eye, hooks[h])
        if last:
            break
        if h == 0:
            joined("a")
        else:
            level_wait(h, "column")
            finish(f"e{h}")
        first = block_value(h, (h + 1, h))
        below[h] = {h + 1: first}
        weights[h + 1, h] = coarse(first, inverses[h], NN)
        if h:
            level_wait(h, "rest")
        span = places[h + 1][h + 1, h + 1]
        ref[f"send{h + 1}"][span] = level_change(h, (h + 1, h + 1))
        level_send(h + 1, "head", span.start, span.stop)
        if h + 2 < levels:
            if h == 0:
                solved_send(0)
                gather("d")
                step("e1")
                plain_part()
                step("e2")
                solved_send(1)
                joined("d")
            for i in range(h + 2, levels):
                below[h][i] = block_value(h, (i, h))
            level_column(h)
            if h == 0:
                hooks[1][1] = [lambda: level_rest(0)]
                hooks[1][2] = [lambda: level_rest_send(0)]
            else:
                level_rest(h)
                level_rest_send(h)
        if h == 0:
            term_sum()
            if levels == 2:
                solved_send(0)
                solved_send(1)
                plain_part()
        if h or levels == 2:
            if h == 0:
                term_joined()
            if h == levels - 2:
                step("e2")
                plain_cross()
                invert_order()
            level_terms(h)
            terms_send(h)
        if h == levels - 2:
            for k in reversed(range(levels - 1)):
                carry[k] = weights[levels - 1, k]
                partial[k] = term_weights[k]
                for j in range(k + 1, levels - 1):
                    carry[k] = carry[k] - fine(carry[j], weights[j, k], NN)
                    partial[k] = partial[k] - fine(partial[j], weights[j, k], NN)
            solved_relay()
    level_terms(levels - 1)
    plain_sum()

    coefficients = [term_weights[levels - 1] if h == levels - 1 else partial[h] for h in range(levels)]
    for h in range(levels - 1):
        coefficients[h] = coefficients[h] - coarse(coefficients[levels - 1], carry[h], NN)
    stack = jnp.concatenate(split(jnp.concatenate(coefficients, 1), 2), 0)
    by_0 = dot(stack, ref["y0"][...], NN)
    by_1 = dot(stack[:own_rows], ref["y1"][...], NN)
    tree_rows = ref["x"][...] - (by_0[:own_rows] + (by_0[own_rows:] + by_1))
    out_ref[...] = permute(tree_rows, ref["back"][...])

    for copy in pool.values():
        copy.wait_send()


def scratch_list(cfg):
    leaves, groups, levels, rank, own_rows, points, piece = cfg
    chips = groups - 1
    width = levels * rank
    direct, slow = direct_units(levels), slow_units(levels)
    items = [
        ("rs", pltpu.VMEM((own_rows, points), F32)),
        ("g", pltpu.VMEM((points, piece), F32)),
        ("b", pltpu.VMEM((levels, rank, points), BF16)),
        ("ord", pltpu.VMEM((1, points), jnp.int32)),
        ("y", pltpu.VMEM((groups, width, piece), F32)),
        ("y0", pltpu.VMEM((width, points), BF16)),
        ("y1", pltpu.VMEM((width, points), BF16)),
        ("x", pltpu.VMEM((own_rows, points), F32)),
        ("tree", pltpu.VMEM((groups, own_rows, piece), F32)),
        ("cols", pltpu.VMEM((groups, own_rows, piece), F32)),
        ("cols_get", pltpu.VMEM((groups - 1, own_rows, piece), F32)),
        ("plain", pltpu.VMEM((2, groups // 2, own_rows, points), F32)),
        ("plain_fold", pltpu.VMEM((groups // 2, own_rows, points), F32)),
        ("plain_chip", pltpu.VMEM((groups // 2, own_rows, points), F32)),
        ("plain_get", pltpu.VMEM((max(1, groups // 2 - 1), own_rows, points), F32)),
        ("term", pltpu.VMEM((2, groups // 2, own_rows, width), F32)),
        ("term_fold", pltpu.VMEM((groups // 2, own_rows, width), F32)),
        ("term_chip", pltpu.VMEM((groups // 2, own_rows, width), F32)),
        ("term_get", pltpu.VMEM((max(1, groups // 2 - 1), own_rows, width), F32)),
        ("term_pass", pltpu.VMEM((own_rows, width), F32)),
        ("term_come", pltpu.VMEM((own_rows, width), F32)),
        ("g0", pltpu.VMEM((points, piece), BF16)),
        ("g1", pltpu.VMEM((points, piece), BF16)),
        ("g2", pltpu.VMEM((points, piece), BF16)),
        ("perm", pltpu.VMEM((points, points), BF16)),
        ("back", pltpu.VMEM((1, points), jnp.int32)),
    ]
    count = 6 + 3 * (groups // 2) - 2 + 4 * (levels - 1) - 2 * (levels > 1)
    for name, blocks in [*direct.items(), *slow.items()]:
        height = layout(blocks, rank)[1]
        items += [
            ("part_" + name, pltpu.VMEM((height, rank), F32)),
            ("fold_" + name, pltpu.VMEM((height // 2, rank), F32)),
            ("full_" + name, pltpu.VMEM((height, rank), F32)),
        ]
        if name in direct:
            count += 3
            items += [
                ("chip_" + name, pltpu.VMEM((height // 2, rank), F32)),
                ("peer_" + name, pltpu.VMEM((chips, height // 2, rank), F32)),
            ]
        else:
            stages = len(stages_of(name, groups))
            count += 2 + stages
            items += [
                ("pass_" + name, pltpu.VMEM((stages, height // 2, rank), F32)),
                ("come_" + name, pltpu.VMEM((stages, height // 2, rank), F32)),
            ]
    for h in range(1, levels):
        height = layout(blocks_of(levels, h), rank)[1]
        items.append((f"send{h}", pltpu.VMEM((height, rank), F32)))
        items.append((f"get{h}", pltpu.VMEM((height, rank), F32)))
        height = (levels - h) * own_rows
        items.append((f"tsend{h}", pltpu.VMEM((height, rank), F32)))
        items.append((f"tget{h}", pltpu.VMEM((height, rank), F32)))
    items.append(("sent", pltpu.SemaphoreType.DMA((POOL + 3 * (groups // 2) - 1,))))
    items.append(("received", pltpu.SemaphoreType.DMA((count,))))
    return items


def scratch_names(cfg):
    return [name for name, _ in scratch_list(cfg)]


def local(right_sides, leaf_inverse, bases, ordering):
    own_rows, points = right_sides.shape
    levels, rank = bases.shape[:2]
    cfg = (
        lax.axis_size("leaf"),
        lax.axis_size("rhs"),
        levels,
        rank,
        own_rows,
        points,
        leaf_inverse.shape[1],
    )
    return pl.pallas_call(
        functools.partial(kernel, cfg),
        out_shape=pltpu.VMEM((own_rows, points), F32),
        in_specs=[pl.BlockSpec(memory_space=pl.ANY)] * 4,
        out_specs=pl.BlockSpec(memory_space=pltpu.VMEM),
        scratch_shapes=[item for _, item in scratch_list(cfg)],
        compiler_params=pltpu.CompilerParams(collective_id=0, has_side_effects=True),
        name="tree_solve",
    )(right_sides, leaf_inverse, bases, ordering)


def solution(mesh):
    placed = (P("rhs", "leaf"), P("leaf", "rhs"), P(None, None, "leaf"), P("leaf", None))
    return jax.shard_map(
        local, mesh=mesh, in_specs=placed, out_specs=P("rhs", "leaf"), check_vma=False
    )
```

```python
import functools
import itertools

import jax
import jax.numpy as jnp
from jax import lax
from jax.experimental import pallas as pl
from jax.experimental.pallas import tpu as pltpu
from jax.sharding import PartitionSpec as P

F32 = jnp.float32
BF16 = jnp.bfloat16
NN = (((1,), (0,)), ((), ()))
NT = (((1,), (1,)), ((), ()))
PANEL = 16
CHUNKS = 4
POOL = 12
ROWS, LANES = 8, 128
RADIX = 32


def split(value, pieces):
    parts = []
    for _ in range(pieces):
        head = value.astype(BF16)
        parts.append(head)
        value = value - head.astype(F32)
    return parts


def dot(left, right, dims):
    return lax.dot_general(left, right, dims, preferred_element_type=F32)


def fine(left, right, dims):
    return lax.dot_general(
        left, right, dims, precision=lax.Precision.HIGHEST, preferred_element_type=F32
    )


def coarse(left, right, dims):
    first, second = split(left, 2)
    upper, lower = split(right, 2)
    return dot(first, upper, dims) + (dot(second, upper, dims) + dot(first, lower, dims))


def inverse(matrix, hooks):
    size = matrix.shape[0]
    count = size // PANEL
    lane = lax.broadcasted_iota(jnp.int32, (PANEL, size), 1)
    row = lax.broadcasted_iota(jnp.int32, (PANEL, size), 0)
    zero = jnp.zeros((PANEL, size), F32)
    panels = [matrix[i * PANEL : (i + 1) * PANEL] for i in range(count)]

    def spread(panel, column):
        return jnp.broadcast_to(panel[:, column : column + 1], (PANEL, size))

    for i in range(count):
        for hook in hooks.get(i, ()):
            hook()
        start = i * PANEL
        inside = (lane >= start) & (lane < start + PANEL)
        panel = panels[i]
        columns = [spread(panel, start + k) for k in range(PANEL)]
        ahead = i + 1 < count
        if ahead:
            next_columns = [spread(panels[i + 1], start + k) for k in range(PANEL)]
        panel = jnp.where(inside, jnp.where(lane - start == row, 1.0, 0.0), panel)
        for k in range(PANEL):
            scale = 1.0 / columns[k][k : k + 1]
            at = row == k
            factor = jnp.where(at, -1.0, columns[k])
            panel = jnp.where(at, 0.0, panel) - factor * (panel[k : k + 1] * scale)
            for j in range(k + 1, PANEL):
                pivot = columns[j][k : k + 1] * scale
                columns[j] = jnp.where(at, 0.0, columns[j]) - factor * pivot
        padded = jnp.concatenate([zero] * i + [panel] + [zero] * (count - 1 - i), 0)
        update = coarse(jnp.concatenate(panels, 0), padded, NN)
        if ahead:
            change = next_columns[0] * panel[0:1]
            for k in range(1, PANEL):
                change = change + next_columns[k] * panel[k : k + 1]
        for j in range(count):
            if j == i:
                panels[j] = panel
            else:
                own = update[j * PANEL : (j + 1) * PANEL]
                own = change if j == i + 1 else own
                panels[j] = jnp.where(inside, 0.0, panels[j]) - own
    return jnp.concatenate(panels, 0)


def blocks_of(levels, first):
    later = [(i, first) for i in range(first + 1, levels)]
    for j in range(first + 1, levels):
        later += [(i, j) for i in range(j, levels)]
    return [(first, first)] + later


def permute(value, index):
    tile = (ROWS, LANES)
    width = value.shape[1]
    bands = []
    for top in range(0, value.shape[0], ROWS):
        out = []
        for left in range(0, width, LANES):
            own = jnp.broadcast_to(index[:, left : left + LANES], tile)
            lane, block = lax.rem(own, LANES), lax.div(own, LANES)
            taken = None
            for source in range(width // LANES):
                part = value[top : top + ROWS, source * LANES : (source + 1) * LANES]
                part = jnp.take_along_axis(part, lane, axis=1)
                taken = part if taken is None else jnp.where(block == source, part, taken)
            out.append(taken)
        bands.append(jnp.concatenate(out, 1))
    return jnp.concatenate(bands, 0)


def layout(blocks, rank):
    spans, start = {}, 0
    for i, j in blocks:
        stop = start + (rank // 8 * 5 if i == j else rank)
        spans[i, j] = slice(start, stop)
        start = stop
    return spans, start


def pack(matrix):
    quarter = matrix.shape[0] // 4
    lane = lax.broadcasted_iota(jnp.int32, (1, 4 * quarter), 1)
    zero, one, two, three = (matrix[k * quarter : (k + 1) * quarter] for k in range(4))
    two = jnp.where(lane < 3 * quarter, two, pltpu.roll(zero, 3 * quarter, 1))
    low, high = one[: quarter // 2], one[quarter // 2 :]
    one = jnp.where(lane < 2 * quarter, low, pltpu.roll(high, 2 * quarter, 1))
    return jnp.concatenate([three, two, one], 0)


def unpack(packed):
    quarter = packed.shape[1] // 4
    three, two = packed[:quarter], packed[quarter : 2 * quarter]
    low = packed[2 * quarter :]
    lower = jnp.concatenate(
        [pltpu.roll(two, quarter, 1), low, pltpu.roll(low, 2 * quarter, 1), two, three], 0
    )
    upper = lower.T
    row = lax.broadcasted_iota(jnp.int32, (4 * quarter, 4 * quarter), 0)
    lane = lax.broadcasted_iota(jnp.int32, (4 * quarter, 4 * quarter), 1)
    return jnp.where(lane // quarter > row // quarter, upper, lower)


def direct_units(levels):
    units = {"c": [(0, 0)]}
    if levels > 1:
        units["a"] = [(1, 0), (1, 1)]
    if levels > 2:
        units["d"] = [(i, 0) for i in range(2, levels)]
    return units


def slow_units(levels):
    units = {}
    if levels > 2:
        units["e1"] = [(i, 1) for i in range(2, levels)]
    for j in range(2, levels):
        units[f"e{j}"] = [(i, j) for i in range(j, levels)]
    return units


def stages_of(name, groups):
    column = int(name[1:])
    stages = [(1 << h, 0) for h in range(1, column + 1)]
    stages += [(0, 1 << k) for k in range(1, groups.bit_length() - 1)]
    return stages + [(1, 0)]


def other(index, bit):
    return index + bit - 2 * bit * ((index // max(bit, 1)) % 2)


def kernel(cfg, rs_hbm, g_hbm, b_hbm, ord_hbm, out_ref, *scratch):
    leaves, groups, levels, rank, own_rows, points, piece = cfg
    rows = groups * own_rows
    ref = dict(zip(scratch_names(cfg), scratch))
    leaf, position = lax.axis_index("leaf"), lax.axis_index("rhs")
    mesh_id = pl.DeviceIdType.MESH
    direct, slow = direct_units(levels), slow_units(levels)

    def at(leaf_index, rhs_index):
        return {"leaf": leaf_index, "rhs": rhs_index}

    rhs_peers = [lax.rem(position + k, groups) for k in range(1, groups)]
    mate = other(position, 1)
    half = lax.rem(position, 2)
    chips = [(leaf, lax.rem(position + k, groups)) for k in range(2, groups, 2)]
    across = [peer for _, peer in chips]
    chips += [(other(leaf, 1), lax.rem(position + k, groups)) for k in range(0, groups, 2)]
    greeted = [(leaf, p) for p in rhs_peers]
    greeted += chips[groups // 2 - 1 :]
    greeted += [(other(leaf, 1 << h), position) for h in range(1, levels)]

    rs_ref, g_ref, b_ref, ord_ref = (ref[name] for name in ("rs", "g", "b", "ord"))
    chunk = points // CHUNKS
    moves = [(b_hbm.at[0], b_ref.at[0])]
    for k in range(CHUNKS):
        span = pl.ds(k * chunk, chunk)
        moves.append((g_hbm.at[span], g_ref.at[span]))
    moves += [(ord_hbm, ord_ref), (rs_hbm, rs_ref)]
    if levels > 1:
        later = pl.ds(1, levels - 1)
        moves.append((b_hbm.at[later], b_ref.at[later]))
    loads = [
        pltpu.make_async_copy(src, dst, ref["sent"].at[POOL - 1 - k]) for k, (src, dst) in enumerate(moves)
    ]
    urgent = CHUNKS + 1
    for load in loads[:urgent]:
        load.start()
    barrier = pltpu.get_barrier_semaphore()
    for target in greeted:
        pl.semaphore_signal(barrier, inc=1, device_id=at(*target), device_id_type=mesh_id)

    pool = {}
    turn = itertools.count()
    slots = itertools.count()

    def start(src, dst, target, receive, place):
        if place in pool:
            pool[place].wait_send()
        copy = pltpu.make_async_remote_copy(
            src_ref=src,
            dst_ref=dst,
            send_sem=ref["sent"].at[place],
            recv_sem=ref["received"].at[receive],
            device_id=at(*target),
            device_id_type=mesh_id,
        )
        copy.start()
        pool[place] = copy
        return copy

    def send(src, dst, target):
        return start(src, dst, target, next(slots), next(turn) % POOL)

    class Group:
        def __init__(self, copies, landed):
            receive = next(slots)
            for src, dst, target in copies:
                start(src, dst, target, receive, next(turn) % POOL)
            self.wait = pltpu.make_async_copy(landed, landed, ref["received"].at[receive])

        def wait_recv(self):
            self.wait.wait()

    def halves(buffer, which):
        count = buffer.shape[0] // 2
        return buffer.at[pl.ds(pl.multiple_of(which * count, count), count)]

    flying = {}

    def fold(name):
        part = halves(ref["part_" + name], 1 - half)
        flying[name] = send(part, ref["fold_" + name], (leaf, mate))

    def folded(name):
        flying[name].wait_recv()
        return halves(ref["part_" + name], half)[...] + ref["fold_" + name][...]

    def join(name, total):
        own = halves(ref["full_" + name], half)
        own[...] = total
        flying[name] = send(own, own, (leaf, mate))

    def scatter(name):
        ref["chip_" + name][...] = folded(name)
        peers = ref["peer_" + name]
        copies = [(ref["chip_" + name], peers.at[k], target) for k, target in enumerate(chips)]
        flying[name] = Group(copies, peers)

    def gather(name):
        total = ref["chip_" + name][...]
        flying[name].wait_recv()
        for k in range(len(chips)):
            total = total + ref["peer_" + name][k]
        join(name, total)

    def joined(name):
        flying[name].wait_recv()

    def slow_step(name, stage):
        stages = stages_of(name, groups)
        if stage == 0:
            total = folded(name)
        else:
            total = ref["pass_" + name][stage - 1]
            flying[name].wait_recv()
            total = total + ref["come_" + name][stage - 1]
        if stage == len(stages):
            join(name, total)
            return
        ref["pass_" + name][stage] = total
        leaf_bit, rhs_bit = stages[stage]
        target = (other(leaf, leaf_bit), other(position, rhs_bit))
        flying[name] = send(ref["pass_" + name].at[stage], ref["come_" + name].at[stage], target)

    todo = {}
    for name in slow:
        count = len(stages_of(name, groups))
        todo[name] = [functools.partial(slow_step, name, k) for k in range(count + 1)]
        todo[name].append(functools.partial(joined, name))

    def step(name, count=1):
        for _ in range(count):
            if todo.get(name):
                todo[name].pop(0)()

    def finish(name):
        while todo.get(name):
            step(name)

    own_cols = pl.ds(pl.multiple_of(position * piece, piece), piece)
    own_y = ref["y"].at[position]

    def products(left, parts):
        return dot(left, parts[0], NN) + dot(left, parts[1], NN)

    def gram_of(solved, first, width):
        own_y[first * rank : first * rank + solved.shape[0]] = solved
        right = b_ref[:width, :, own_cols].reshape(width * rank, piece)
        return sum(dot(part, right, NT) for part in reversed(split(solved, 2)))

    def solved_of(first, last):
        left = b_ref[first:last].reshape((last - first) * rank, points)
        return products(left, [ref[f"g{k}"][...] for k in range(2)])

    loads[0].wait()
    solved = None
    for c in range(CHUNKS):
        loads[1 + c].wait()
        if c == CHUNKS // 2:
            loads[-1].start()
        if c == CHUNKS - 1:
            for load in loads[urgent : urgent + 2]:
                load.start()
        span = slice(c * chunk, (c + 1) * chunk)
        parts = split(g_ref[span], 3)
        for k, part in enumerate(parts):
            ref[f"g{k}"][span] = part
        value = products(b_ref[0, :, span], parts)
        solved = value if c == 0 else solved + value
    ref["part_c"][...] = pack(gram_of(solved, 0, 1))
    pl.semaphore_wait(barrier, len(greeted))
    fold("c")

    def arrange():
        for load in loads[urgent : urgent + 2]:
            load.wait()
        tree = permute(rs_ref[...], ord_ref[...])
        for k in range(groups):
            ref["tree"][k] = tree[:, k * piece : (k + 1) * piece]

    def invert_order():
        order = ord_ref[...]

        def one_hot(i, carry):
            start = pl.multiple_of(i * rank, rank)
            index = lax.broadcasted_iota(jnp.int32, (rank, points), 0) + start
            ref["perm"][pl.ds(start, rank), :] = jnp.where(index == order, 1.0, 0.0).astype(BF16)
            return carry

        lax.fori_loop(0, points // rank, one_hot, 0)
        row = lax.broadcasted_iota(jnp.int32, (2 * ROWS, points), 0)
        lane = lax.broadcasted_iota(jnp.int32, (2 * ROWS, points), 1)
        digits = jnp.where(row == 0, lax.div(lane, RADIX), lax.rem(lane, RADIX))
        found = dot(digits.astype(F32).astype(BF16), ref["perm"][...], NT)
        ref["back"][...] = (found[:1] * RADIX + found[1:2]).astype(jnp.int32)

    def part_store(gram, start, name, blocks):
        for (i, j), span in layout(blocks, rank)[0].items():
            block = gram[(i - start) * rank : (i - start + 1) * rank, j * rank : (j + 1) * rank]
            ref["part_" + name][span] = pack(block) if i == j else block

    if levels > 1:
        loads[urgent + 2].wait()
        solved = solved_of(1, 2)
    scatter("c")
    if levels > 1:
        part_store(gram_of(solved, 1, 2), 1, "a", direct["a"])
        fold("a")
    arrange()
    ref["cols"][position] = ref["tree"][position]
    copies = [
        (ref["tree"].at[peer], ref["cols_get"].at[k], (leaf, peer))
        for k, peer in enumerate(rhs_peers)
    ]
    pieces = Group(copies, ref["cols_get"])
    if levels > 2:
        gram = gram_of(solved_of(2, levels), 2, levels)
        later = {name: blocks for name, blocks in direct.items() if name not in "ca"}
        later |= slow
        for name, blocks in later.items():
            part_store(gram, 2, name, blocks)
        scatter("a")
        for name in later:
            fold(name)
    elif levels > 1:
        scatter("a")

    terms = []

    def term_part():
        pieces.wait_recv()
        for k in range(groups - 1):
            source = lax.rem(position + groups - 1 - k, groups)
            ref["cols"][source] = ref["cols_get"][k]
        columns = ref["cols"][...].reshape(rows, piece)
        term = fine(columns, own_y[...], NT)
        for k in range(groups):
            ref["term"][k % 2, k // 2] = term[k * own_rows : (k + 1) * own_rows]
        terms.append(send(ref["term"].at[1 - half], ref["term_fold"], (leaf, mate)))

    def term_cross():
        terms[0].wait_recv()
        ref["term_chip"][...] = ref["term"][half] + ref["term_fold"][...]
        for k, peer in enumerate(across):
            source = ref["term_chip"].at[lax.div(peer, 2)]
            terms.append(send(source, ref["term_get"].at[k], (leaf, peer)))

    def term_sum():
        total = ref["term_chip"][lax.div(position, 2)]
        for k, copy in enumerate(terms[1:]):
            copy.wait_recv()
            total = total + ref["term_get"][k]
        ref["term_pass"][...] = total
        terms.append(send(ref["term_pass"], ref["term_come"], (other(leaf, 1), position)))

    def term_joined():
        terms[-1].wait_recv()

    plain = []

    def plain_part():
        stack = jnp.concatenate(split(ref["cols"][...].reshape(rows, piece), 3), 0)
        by_0 = dot(stack, ref["g0"][...], NT)
        by_1 = dot(stack[: 2 * rows], ref["g1"][...], NT)
        by_2 = dot(stack[:rows], ref["g2"][...], NT)
        value = by_0[:rows] + (
            (by_0[rows : 2 * rows] + by_1[:rows]) + (by_0[2 * rows :] + by_1[rows:] + by_2)
        )
        for k in range(groups):
            ref["plain"][k % 2, k // 2] = value[k * own_rows : (k + 1) * own_rows]
        plain.append(send(ref["plain"].at[1 - half], ref["plain_fold"], (leaf, mate)))

    def plain_cross():
        plain[0].wait_recv()
        ref["plain_chip"][...] = ref["plain"][half] + ref["plain_fold"][...]
        for k, peer in enumerate(across):
            source = ref["plain_chip"].at[lax.div(peer, 2)]
            plain.append(send(source, ref["plain_get"].at[k], (leaf, peer)))

    def plain_sum():
        total = ref["plain_chip"][lax.div(position, 2)]
        for k, copy in enumerate(plain[1:]):
            copy.wait_recv()
            total = total + ref["plain_get"][k]
        ref["x"][...] = total

    solved_copies, relays = [], []

    def solved_across(first, last, place):
        part = own_y.at[pl.ds(first, last - first)]
        for k, peer in enumerate(across):
            solved_copies.append(start(part, part, (leaf, peer), next(slots), place + k))

    def solved_send(part):
        early = rank // 2
        if part == 0:
            solved_across(0, early, POOL)
        else:
            solved_across(early, levels * rank, POOL + len(across))
            place = POOL + 2 * len(across)
            relays.append(start(own_y, own_y, (leaf, mate), next(slots), place))

    def solved_relay():
        for copy in solved_copies:
            copy.wait_recv()
        for k in range(len(across)):
            source = lax.rem(position + groups - 2 * (k + 1), groups)
            slot = ref["y"].at[source]
            place = POOL + 2 * len(across) + 1 + k
            relays.append(start(slot, slot, (leaf, mate), next(slots), place))

    def solved_done():
        for copy in relays:
            copy.wait_recv()
        for k in range(groups):
            for p, part in enumerate(split(ref["y"][k], 2)):
                ref[f"y{p}"][:, k * piece : (k + 1) * piece] = part

    eye = (
        lax.broadcasted_iota(jnp.int32, (rank, rank), 0)
        == lax.broadcasted_iota(jnp.int32, (rank, rank), 1)
    ).astype(F32)
    linear = {}
    for name, blocks in [*direct.items(), *slow.items()]:
        for block, span in layout(blocks, rank)[0].items():
            linear[block] = (name, span)
    places = [layout(blocks_of(levels, h), rank)[0] for h in range(levels)]

    def linear_value(block):
        name, span = linear[block]
        return ref["full_" + name][span]

    def carried(h, block):
        span = places[h][block]
        return ref[f"send{h}"][span] + ref[f"get{h}"][span]

    def block_value(h, block):
        if h == 0:
            return linear_value(block)
        value = carried(h, block)
        return value if block == (1, 1) else value + linear_value(block)

    def term_value(h, j):
        if h == 0:
            span = slice(j * rank, (j + 1) * rank)
            return ref["term_pass"][:, span] + ref["term_come"][:, span]
        start = (j - h) * own_rows
        span = slice(start, start + own_rows)
        return ref[f"tsend{h}"][span] + ref[f"tget{h}"][span]

    level_copies = {}

    def level_send(h, part, start, stop):
        span = pl.ds(start, stop - start)
        level_copies[h, part] = send(
            ref[f"send{h}"].at[span], ref[f"get{h}"].at[span], (other(leaf, 1 << h), position)
        )

    def level_wait(h, part):
        copy = level_copies.pop((h, part), None)
        if copy is not None:
            copy.wait_recv()

    inverses = [None] * levels
    below = [None] * levels
    weights = {}
    term_weights = {}

    def level_terms(h):
        if h:
            level_wait(h, "terms")
        own = term_value(h, h)
        term_weights[h] = coarse(own, inverses[h], NN)
        if h + 1 < levels:
            for k, j in enumerate(range(h + 1, levels)):
                change = coarse(own, weights[j, h], NT)
                span = slice(k * own_rows, (k + 1) * own_rows)
                ref[f"tsend{h + 1}"][span] = term_value(h, j) - change

    def terms_send(h):
        level_copies[h + 1, "terms"] = send(
            ref[f"tsend{h + 1}"], ref[f"tget{h + 1}"], (other(leaf, 2 << h), position)
        )

    def level_change(h, block):
        i, j = block
        change = coarse(weights[i, h], below[h][j], NT)
        if i == j:
            change = pack(change)
        if block == (1, 1):
            return linear_value(block) - change
        return carried(h, block) - change if h else -change

    def level_span(h, first, last):
        return [(block, places[h][block]) for block in blocks_of(levels, h)[first:last]]

    def level_column(h):
        level_wait(h, "rest")
        spans = level_span(h + 1, 1, levels - h - 1)
        for (i, j), span in spans:
            change = coarse(below[h][i], weights[j, h], NT)
            ref[f"send{h + 1}"][span] = carried(h, (i, j)) - change if h else -change
        level_send(h + 1, "column", spans[0][1].start, spans[-1][1].stop)

    def level_rest(h):
        for i in range(h + 2, levels):
            weights[i, h] = coarse(below[h][i], inverses[h], NN)
        for block, span in level_span(h + 1, levels - h - 1, None):
            ref[f"send{h + 1}"][span] = level_change(h, block)

    def level_rest_send(h):
        spans = level_span(h + 1, levels - h - 1, None)
        level_send(h + 1, "rest", spans[0][1].start, spans[-1][1].stop)


    for name in slow:
        step(name)
    gather("c")
    term_part()
    joined("c")
    hooks = {h: {} for h in range(levels)}
    if levels > 1:
        hooks[0] = {5: [lambda: gather("a")]}
    if levels > 2:
        hooks[0][1] = [lambda: scatter("d")]
        hooks[0][3] = [term_cross]
        hooks[0][4] = [lambda: step("e1"), lambda: step("e2")]
        hooks[1] = {
            3: [lambda: step("e1")],
            5: [lambda: step("e2"), term_joined, lambda: level_terms(0)],
            6: [lambda: terms_send(0)],
        }
    else:
        hooks[0][2] = [term_cross]
    carry, partial = [None] * levels, [None] * levels
    for h in range(levels):
        last = h == levels - 1
        if h:
            level_wait(h, "head")
            if h > 1:
                finish(f"e{h}")
        if last:
            if h == 0:
                term_sum()
                solved_send(0)
                solved_send(1)
                plain_part()
                plain_cross()
                term_joined()
                solved_relay()
                invert_order()
            hooks[h][7] = [solved_done]
        inverses[h] = inverse(unpack(block_value(h, (h, h))) + eye, hooks[h])
        if last:
            break
        if h == 0:
            joined("a")
        else:
            level_wait(h, "column")
            finish(f"e{h}")
        first = block_value(h, (h + 1, h))
        below[h] = {h + 1: first}
        weights[h + 1, h] = coarse(first, inverses[h], NN)
        if h:
            level_wait(h, "rest")
        span = places[h + 1][h + 1, h + 1]
        ref[f"send{h + 1}"][span] = level_change(h, (h + 1, h + 1))
        level_send(h + 1, "head", span.start, span.stop)
        if h + 2 < levels:
            if h == 0:
                solved_send(0)
                gather("d")
                step("e1")
                plain_part()
                step("e2")
                solved_send(1)
                joined("d")
            for i in range(h + 2, levels):
                below[h][i] = block_value(h, (i, h))
            level_column(h)
            if h == 0:
                hooks[1][1] = [lambda: level_rest(0)]
                hooks[1][2] = [lambda: level_rest_send(0)]
            else:
                level_rest(h)
                level_rest_send(h)
        if h == 0:
            term_sum()
            if levels == 2:
                solved_send(0)
                solved_send(1)
                plain_part()
        if h or levels == 2:
            if h == 0:
                term_joined()
            if h == levels - 2:
                step("e2")
                plain_cross()
                invert_order()
            level_terms(h)
            terms_send(h)
        if h == levels - 2:
            for k in reversed(range(levels - 1)):
                carry[k] = weights[levels - 1, k]
                partial[k] = term_weights[k]
                for j in range(k + 1, levels - 1):
                    carry[k] = carry[k] - fine(carry[j], weights[j, k], NN)
                    partial[k] = partial[k] - fine(partial[j], weights[j, k], NN)
            solved_relay()
    level_terms(levels - 1)
    plain_sum()

    coefficients = [term_weights[levels - 1] if h == levels - 1 else partial[h] for h in range(levels)]
    for h in range(levels - 1):
        coefficients[h] = coefficients[h] - coarse(coefficients[levels - 1], carry[h], NN)
    stack = jnp.concatenate(split(jnp.concatenate(coefficients, 1), 2), 0)
    by_0 = dot(stack, ref["y0"][...], NN)
    by_1 = dot(stack[:own_rows], ref["y1"][...], NN)
    tree_rows = ref["x"][...] - (by_0[:own_rows] + (by_0[own_rows:] + by_1))
    out_ref[...] = permute(tree_rows, ref["back"][...])

    for copy in pool.values():
        copy.wait_send()


def scratch_list(cfg):
    leaves, groups, levels, rank, own_rows, points, piece = cfg
    chips = groups - 1
    width = levels * rank
    direct, slow = direct_units(levels), slow_units(levels)
    items = [
        ("rs", pltpu.VMEM((own_rows, points), F32)),
        ("g", pltpu.VMEM((points, piece), F32)),
        ("b", pltpu.VMEM((levels, rank, points), BF16)),
        ("ord", pltpu.VMEM((1, points), jnp.int32)),
        ("y", pltpu.VMEM((groups, width, piece), F32)),
        ("y0", pltpu.VMEM((width, points), BF16)),
        ("y1", pltpu.VMEM((width, points), BF16)),
        ("x", pltpu.VMEM((own_rows, points), F32)),
        ("tree", pltpu.VMEM((groups, own_rows, piece), F32)),
        ("cols", pltpu.VMEM((groups, own_rows, piece), F32)),
        ("cols_get", pltpu.VMEM((groups - 1, own_rows, piece), F32)),
        ("plain", pltpu.VMEM((2, groups // 2, own_rows, points), F32)),
        ("plain_fold", pltpu.VMEM((groups // 2, own_rows, points), F32)),
        ("plain_chip", pltpu.VMEM((groups // 2, own_rows, points), F32)),
        ("plain_get", pltpu.VMEM((max(1, groups // 2 - 1), own_rows, points), F32)),
        ("term", pltpu.VMEM((2, groups // 2, own_rows, width), F32)),
        ("term_fold", pltpu.VMEM((groups // 2, own_rows, width), F32)),
        ("term_chip", pltpu.VMEM((groups // 2, own_rows, width), F32)),
        ("term_get", pltpu.VMEM((max(1, groups // 2 - 1), own_rows, width), F32)),
        ("term_pass", pltpu.VMEM((own_rows, width), F32)),
        ("term_come", pltpu.VMEM((own_rows, width), F32)),
        ("g0", pltpu.VMEM((points, piece), BF16)),
        ("g1", pltpu.VMEM((points, piece), BF16)),
        ("g2", pltpu.VMEM((points, piece), BF16)),
        ("perm", pltpu.VMEM((points, points), BF16)),
        ("back", pltpu.VMEM((1, points), jnp.int32)),
    ]
    count = 6 + 3 * (groups // 2) - 2 + 4 * (levels - 1) - 2 * (levels > 1)
    for name, blocks in [*direct.items(), *slow.items()]:
        height = layout(blocks, rank)[1]
        items += [
            ("part_" + name, pltpu.VMEM((height, rank), F32)),
            ("fold_" + name, pltpu.VMEM((height // 2, rank), F32)),
            ("full_" + name, pltpu.VMEM((height, rank), F32)),
        ]
        if name in direct:
            count += 3
            items += [
                ("chip_" + name, pltpu.VMEM((height // 2, rank), F32)),
                ("peer_" + name, pltpu.VMEM((chips, height // 2, rank), F32)),
            ]
        else:
            stages = len(stages_of(name, groups))
            count += 2 + stages
            items += [
                ("pass_" + name, pltpu.VMEM((stages, height // 2, rank), F32)),
                ("come_" + name, pltpu.VMEM((stages, height // 2, rank), F32)),
            ]
    for h in range(1, levels):
        height = layout(blocks_of(levels, h), rank)[1]
        items.append((f"send{h}", pltpu.VMEM((height, rank), F32)))
        items.append((f"get{h}", pltpu.VMEM((height, rank), F32)))
        height = (levels - h) * own_rows
        items.append((f"tsend{h}", pltpu.VMEM((height, rank), F32)))
        items.append((f"tget{h}", pltpu.VMEM((height, rank), F32)))
    items.append(("sent", pltpu.SemaphoreType.DMA((POOL + 3 * (groups // 2) - 1,))))
    items.append(("received", pltpu.SemaphoreType.DMA((count,))))
    return items


def scratch_names(cfg):
    return [name for name, _ in scratch_list(cfg)]


def local(right_sides, leaf_inverse, bases, ordering):
    own_rows, points = right_sides.shape
    levels, rank = bases.shape[:2]
    cfg = (
        lax.axis_size("leaf"),
        lax.axis_size("rhs"),
        levels,
        rank,
        own_rows,
        points,
        leaf_inverse.shape[1],
    )
    return pl.pallas_call(
        functools.partial(kernel, cfg),
        out_shape=pltpu.VMEM((own_rows, points), F32),
        in_specs=[pl.BlockSpec(memory_space=pl.ANY)] * 4,
        out_specs=pl.BlockSpec(memory_space=pltpu.VMEM),
        scratch_shapes=[item for _, item in scratch_list(cfg)],
        compiler_params=pltpu.CompilerParams(collective_id=0, has_side_effects=True),
        name="tree_solve",
    )(right_sides, leaf_inverse, bases, ordering)


def solution(mesh):
    placed = (P("rhs", "leaf"), P("leaf", "rhs"), P(None, None, "leaf"), P("leaf", None))
    return jax.shard_map(
        local, mesh=mesh, in_specs=placed, out_specs=P("rhs", "leaf"), check_vma=False
    )
```
